32 devices in a mesh: rep: 1 (over z), dp: 32 (over x, y, core).
Axes of the slice: x: 4, y: 4, z: 1, core: 2. Of those that a mesh axis runs over, the one named last changes fastest.
The devices are a block of a 4x4x8 slice.
Arguments:
- x: bfloat16 [32, 2048, 768], P(('rep', 'dp'))
- dy: bfloat16 [32, 2048, 768], P(('rep', 'dp'))
- w_gate: bfloat16 [2, 768, 2304], replicated
- w_up: bfloat16 [2, 768, 2304], replicated
- w_down: bfloat16 [2, 2304, 768], replicated
- m_w_gate: float32 [2, 768, 2304], replicated
- m_w_up: float32 [2, 768, 2304], replicated
- m_w_down: float32 [2, 2304, 768], replicated
- v_w_gate: float32 [2, 768, 2304], replicated
- v_w_up: float32 [2, 768, 2304], replicated
- v_w_down: float32 [2, 2304, 768], replicated
Outputs:
- output 1: bfloat16 [2, 768, 2304], P('rep')
- output 2: bfloat16 [2, 768, 2304], P('rep')
- output 3: bfloat16 [2, 2304, 768], P('rep')
- output 4: float32 [2, 768, 2304], P('rep')
- output 5: float32 [2, 768, 2304], P('rep')
- output 6: float32 [2, 2304, 768], P('rep')
- output 7: float32 [2, 768, 2304], P('rep')
- output 8: float32 [2, 768, 2304], P('rep')
- output 9: float32 [2, 2304, 768], P('rep')
All inputs are finite; a program needn't handle non-finite values.
Results may differ from the reference program's by a relative error of at most 0.022.
Values are sent between devices in bfloat16 or wider.
A program may use at most 768 MiB of HBM per device.

```python
import jax
import jax.numpy as jnp
from jax import lax

SEQUENCES = 32
TOKENS = 2048
D = 768
FF = 2304
LAYERS = 2
NAMES = ("w_gate", "w_up", "w_down")
SHAPES = {"w_gate": (LAYERS, D, FF), "w_up": (LAYERS, D, FF), "w_down": (LAYERS, FF, D)}


def bump(key, n, height):
    away = (jnp.arange(n, dtype=jnp.int32) - jax.random.randint(key, (), 0, n, jnp.int32)) % n
    return jnp.where(away < n // 8, height, 1.0)


def together(key, own, strength):
    shared = jax.random.normal(key, own.shape[1:], jnp.float32)
    return (own + strength * shared) * lax.rsqrt(1 + strength * strength)


def setup_inputs(seed: int = 0, part: int = 0) -> dict:
    kx, kdy, ka, kb, kz, kf, kh, kl, *keys = jax.random.split(jax.random.key(seed), 8 + 3 * len(NAMES))
    kx, kdy, ka, kb = (jax.random.fold_in(k, part) for k in (kx, kdy, ka, kb))
    kw, km, kv = (keys[i::3] for i in range(3))
    shape = (SEQUENCES, TOKENS, D)
    much_x, much_dy = jax.random.uniform(kz, (2,), jnp.float32, 0.0, 1.0)
    loud = 2.0 ** jax.random.uniform(jax.random.fold_in(kz, 1), (), jnp.float32, -1.0, 2.0)
    layers = 2.0 ** jax.random.uniform(kl, (LAYERS, 1, 1), jnp.float32, -1.0, 1.0)
    x = together(ka, jax.random.normal(kx, shape, jnp.float32), much_x) * bump(kf, D, 4.0)
    dy = together(kb, jax.random.normal(kdy, shape, jnp.float32), much_dy)
    drawn = {"x": x.astype(jnp.bfloat16), "dy": (loud * dy * (SEQUENCES * TOKENS) ** -0.5).astype(jnp.bfloat16)}
    for key, name in zip(kw, NAMES, strict=True):
        w = jax.random.normal(key, SHAPES[name], jnp.float32) * SHAPES[name][1] ** -0.5
        drawn[name] = (w * {"w_gate": 1.0, "w_up": bump(kh, FF, 4.0), "w_down": layers}[name]).astype(jnp.bfloat16)
    for key, name in zip(km, NAMES, strict=True):
        drawn[f"m_{name}"] = 0.1 * jax.random.normal(key, SHAPES[name], jnp.float32)
    for key, name in zip(kv, NAMES, strict=True):
        drawn[f"v_{name}"] = jax.random.uniform(key, SHAPES[name], jnp.float32, 0.005, 0.015)
    return drawn


def matmul(a, w):
    return jnp.dot(a, w, preferred_element_type=jnp.float32).astype(jnp.bfloat16)


def normed(h):
    wide = h.astype(jnp.float32)
    scale = lax.rsqrt(jnp.mean(wide**2, -1, keepdims=True) + 1e-6)
    return (wide * scale).astype(jnp.bfloat16)


def layer(h, w):
    a = normed(h)
    gate = jnp.dot(a, w["w_gate"], preferred_element_type=jnp.float32)
    up = jnp.dot(a, w["w_up"], preferred_element_type=jnp.float32)
    return h + matmul((jax.nn.silu(gate) * up).astype(jnp.bfloat16), w["w_down"])


def adamw(w, m, v, g):
    m = 0.9 * m + 0.1 * g
    v = 0.95 * v + 0.05 * g * g
    step = m * lax.rsqrt(v + 1e-8) + 0.1 * w
    return (w - 0.02 * step).astype(jnp.bfloat16), m, v


def clipped(gradients, sum_of_squares, count):
    factor = jnp.minimum(1.0, 0.5 * lax.rsqrt(sum_of_squares / count + 1e-30))
    return [g * factor for g in gradients]


def stack(weights, h):
    return lax.scan(lambda h, w: (layer(h, w), None), h, weights)[0]


def reference(x, dy, w_gate, w_up, w_down, m_w_gate, m_w_up, m_w_down, v_w_gate, v_w_up, v_w_down):
    weights = dict(zip(NAMES, (w_gate, w_up, w_down), strict=True))

    def take(so_far, sequence):
        h, by_y = sequence
        _, back = jax.vjp(lambda w: stack(w, h), weights)
        return jax.tree.map(lambda total, term: total + term.astype(jnp.float32), so_far, back(by_y)[0]), None

    none_yet = {name: jnp.zeros(w.shape, jnp.float32) for name, w in weights.items()}
    by_weights, _ = lax.scan(take, none_yet, (x, dy))
    gradients = [by_weights[name].astype(jnp.bfloat16).astype(jnp.float32) for name in NAMES]
    gradients = clipped(gradients, sum(jnp.sum(g * g) for g in gradients), sum(g.size for g in gradients))
    new = [
        adamw(w.astype(jnp.float32), m, v, g)
        for w, m, v, g in zip((w_gate, w_up, w_down), (m_w_gate, m_w_up, m_w_down), (v_w_gate, v_w_up, v_w_down), gradients, strict=True)
    ]
    return tuple(one[which] for which in range(3) for one in new)
```

```python
import functools
import jax, jax.numpy as jnp
from jax import lax
from jax.experimental import pallas as pl
from jax.experimental.pallas import tpu as pltpu
from jax.sharding import PartitionSpec as P
F32,BF=jnp.float32,jnp.bfloat16
ANY=pl.BlockSpec(memory_space=pl.ANY)
VM=pl.BlockSpec(memory_space=pltpu.VMEM)
def dot(a,b,dims=((1,),(0,))):
    return lax.dot_general(a,b,(dims,((),())),preferred_element_type=F32)
NT=((1,),(1,)); TN=((0,),(0,))
def norm_scale(wide): return lax.rsqrt(jnp.mean(wide*wide,-1,keepdims=True)+1e-6)
def normed(h):
    wide=h.astype(F32); return (wide*norm_scale(wide)).astype(BF)
def sigmoid(g): return 0.5*jnp.tanh(0.5*g)+0.5

def k1_body(x_ref,wg,wu,wd,gate_ref,up_ref,h_ref,a_ref,act,*,fc):
    x=x_ref[...]; a=normed(x); F=wg.shape[1]
    for c in range(F//fc):
        s=pl.ds(c*fc,fc)
        g=dot(a,wg[:,s]); u=dot(a,wu[:,s])
        gate_ref[:,s]=g; up_ref[:,s]=u
        act[:,s]=(g*sigmoid(g)*u).astype(BF)
    d=dot(act[...],wd[...]).astype(BF)
    h=(x.astype(F32)+d.astype(F32)).astype(BF)
    h_ref[...]=h; a_ref[...]=normed(h)
def k1(x,wg,wu,wd,bm=512,fc=768):
    T,D=x.shape; F=wg.shape[2]
    wspec=lambda r,c:pl.BlockSpec((None,r,c),lambda i:(0,0,0),pipeline_mode=pl.Buffered(1))
    row=lambda c:pl.BlockSpec((bm,c),lambda i:(i,0))
    return pl.pallas_call(functools.partial(k1_body,fc=fc),grid=(T//bm,),
        in_specs=[row(D),wspec(D,F),wspec(D,F),wspec(F,D)],
        out_specs=[row(F),row(F),row(D),row(D)],
        out_shape=[jax.ShapeDtypeStruct((T,F),F32)]*2+[jax.ShapeDtypeStruct((T,D),BF)]*2,
        scratch_shapes=[pltpu.VMEM((bm,F),BF)],
        compiler_params=pltpu.CompilerParams(vmem_limit_bytes=60<<20),name="k1",
        cost_estimate=pl.CostEstimate(flops=6*T*D*F,bytes_accessed=10*T*F,transcendentals=T*F))(x,wg,wu,wd)

def k2_body(a_ref,dy_ref,h_ref,wg_h,wu_h,wd_h,dwg,dwu,dwd,dh_ref,wg,wu,wd,aT,dg,du,act,sem,*,nf,ft,rc,bc):
    j=pl.program_id(0); T,D=a_ref.shape; L=1
    cps=lambda t:[pltpu.make_async_copy(wg_h.at[L,:,pl.ds(t*ft,ft)],wg.at[:,pl.ds(t*ft,ft)],sem.at[0,t]),
                  pltpu.make_async_copy(wu_h.at[L,:,pl.ds(t*ft,ft)],wu.at[:,pl.ds(t*ft,ft)],sem.at[1,t]),
                  pltpu.make_async_copy(wd_h.at[L,pl.ds(t*ft,ft),:],wd.at[pl.ds(t*ft,ft),:],sem.at[2,t])]
    @pl.when(j==0)
    def _():
        for t in range(nf):
            for c in cps(t): c.start()
        for r in range(T//512): aT[:,pl.ds(r*512,512)]=a_ref[pl.ds(r*512,512),:].T
    @pl.when(j<nf)
    def _():
        for c in cps(j): c.wait()
        off=pl.multiple_of(j*ft,ft); s=pl.ds(off,ft)
        wgt,wut,wdt=wg[:,s],wu[:,s],wd[s,:]
        for r in range(T//rc):
            rs=pl.ds(r*rc,rc)
            a=a_ref[rs,:]
            g=dot(a,wgt); u=dot(a,wut); da=dot(dy_ref[rs,:],wdt,NT).astype(BF).astype(F32)
            sg=sigmoid(g); silu=g*sg
            act[rs,:]=(silu*u).astype(BF)
            du[rs,s]=(da*silu).astype(BF)
            dg[rs,s]=(da*u*(sg+silu*(1.0-sg))).astype(BF)
        dwg[...]=dot(aT[...],dg[:,s]).astype(BF)
        dwu[...]=dot(aT[...],du[:,s]).astype(BF)
        dwd[...]=dot(act[...],dy_ref[...],TN).astype(BF)
    @pl.when(j>=nf)
    def _():
        r=pl.multiple_of((j-nf)*bc,bc); rs=pl.ds(r,bc)
        da=(dot(dg[rs,:],wg[...],NT).astype(BF).astype(F32)+dot(du[rs,:],wu[...],NT).astype(BF).astype(F32)).astype(BF).astype(F32)
        wide=h_ref[rs,:].astype(F32); sc=norm_scale(wide)
        t=jnp.sum(da*wide,-1,keepdims=True)*(1.0/D)
        dn=(da*sc-wide*(sc*sc*sc*t)).astype(BF).astype(F32)
        dh_ref[rs,:]=(dy_ref[rs,:].astype(F32)+dn).astype(BF)
def k2(a1,dy,h1,wg,wu,wd,ft=256,rc=512,bc=512):
    T,D=a1.shape; F=wg.shape[2]; nf=F//ft; nb=T//bc
    col=pl.BlockSpec((D,ft),lambda j:(0,jnp.minimum(j,nf-1))); rowb=pl.BlockSpec((ft,D),lambda j:(jnp.minimum(j,nf-1),0))
    return pl.pallas_call(functools.partial(k2_body,nf=nf,ft=ft,rc=rc,bc=bc),grid=(nf+nb,),
        in_specs=[VM,VM,VM,ANY,ANY,ANY],out_specs=[col,col,rowb,pl.BlockSpec((T,D),lambda j:(0,0))],
        out_shape=[jax.ShapeDtypeStruct((D,F),BF)]*2+[jax.ShapeDtypeStruct((F,D),BF),jax.ShapeDtypeStruct((T,D),BF)],
        scratch_shapes=[pltpu.VMEM((D,F),BF),pltpu.VMEM((D,F),BF),pltpu.VMEM((F,D),BF),pltpu.VMEM((D,T),BF),
                        pltpu.VMEM((T,F),BF),pltpu.VMEM((T,F),BF),pltpu.VMEM((T,ft),BF),pltpu.SemaphoreType.DMA((3,nf))],
        compiler_params=pltpu.CompilerParams(vmem_limit_bytes=63<<20),name="k2",
        cost_estimate=pl.CostEstimate(flops=16*T*D*F,bytes_accessed=30<<20,transcendentals=T*F))(a1,dy,h1,wg,wu,wd)

def k3_body(x_ref,dh_ref,g_ref,u_ref,wd_ref,dwg,dwu,dwd,aT,dg,du,act,*,rc):
    j=pl.program_id(0); T,D=x_ref.shape
    @pl.when(j==0)
    def _():
        for r in range(T//512): aT[:,pl.ds(r*512,512)]=normed(x_ref[pl.ds(r*512,512),:]).T
    wdt=wd_ref[...]
    for r in range(T//rc):
        rs=pl.ds(r*rc,rc)
        da=dot(dh_ref[rs,:],wdt,NT).astype(BF).astype(F32)
        g=g_ref[rs,:]; u=u_ref[rs,:]
        sg=sigmoid(g); silu=g*sg
        act[rs,:]=(silu*u).astype(BF)
        du[rs,:]=(da*silu).astype(BF)
        dg[rs,:]=(da*u*(sg+silu*(1.0-sg))).astype(BF)
    dwg[...]=dot(aT[...],dg[...]).astype(BF)
    dwu[...]=dot(aT[...],du[...]).astype(BF)
    dwd[...]=dot(act[...],dh_ref[...],TN).astype(BF)
def k3(x,dh,gate,up,wd,ft=256,rc=512):
    T,D=x.shape; F=gate.shape[1]; nf=F//ft
    col=lambda r:pl.BlockSpec((r,ft),lambda j:(0,j))
    return pl.pallas_call(functools.partial(k3_body,rc=rc),grid=(nf,),
        in_specs=[VM,VM,col(T),col(T),pl.BlockSpec((None,ft,D),lambda j:(0,j,0))],
        out_specs=[col(D),col(D),pl.BlockSpec((ft,D),lambda j:(j,0))],
        out_shape=[jax.ShapeDtypeStruct((D,F),BF)]*2+[jax.ShapeDtypeStruct((F,D),BF)],
        scratch_shapes=[pltpu.VMEM((D,T),BF)]+[pltpu.VMEM((T,ft),BF)]*3,
        compiler_params=pltpu.CompilerParams(vmem_limit_bytes=60<<20),name="k3",
        cost_estimate=pl.CostEstimate(flops=8*T*D*F,bytes_accessed=10*T*F,transcendentals=T*F))(x,dh,gate,up,wd)


def adamw(w, m, v, g):
    m = 0.9 * m + 0.1 * g
    v = 0.95 * v + 0.05 * g * g
    step = m * lax.rsqrt(v + 1e-8) + 0.1 * w
    return (w - 0.02 * step).astype(jnp.bfloat16), m, v


def clipped(gradients, sum_of_squares, count):
    factor = jnp.minimum(1.0, 0.5 * lax.rsqrt(sum_of_squares / count + 1e-30))
    return [g * factor for g in gradients]


def solution(mesh):
    def step(x, dy, *arrays):
        weights, m, v = (arrays[i : i + 3] for i in (0, 3, 6))
        gate, up, h1, a1 = k1(x[0], *weights)
        *of1, dh = k2(a1, dy[0], h1, *weights)
        of0 = k3(x[0], dh, gate, up, weights[2])
        summed = [[lax.psum(g, "dp") for g in one] for one in (of0, of1)]
        gradients = [jnp.stack([one[i] for one in summed]).astype(F32) for i in range(3)]
        gradients = clipped(gradients, sum(jnp.sum(g * g) for g in gradients), sum(g.size for g in gradients))
        new = [adamw(w.astype(F32), m, v, g) for w, m, v, g in zip(weights, m, v, gradients, strict=True)]
        return tuple(one[which] for which in range(3) for one in new)

    return jax.shard_map(
        step,
        mesh=mesh,
        in_specs=(P(("rep", "dp"), None, None),) * 2 + (P(None, None, None),) * 9,
        out_specs=(P("rep", None, None),) * 9,
        check_vma=False,
    )
```

```python
import functools
import jax, jax.numpy as jnp
from jax import lax
from jax.experimental import pallas as pl
from jax.experimental.pallas import tpu as pltpu
from jax.sharding import PartitionSpec as P
F32,BF=jnp.float32,jnp.bfloat16
ANY=pl.BlockSpec(memory_space=pl.ANY)
VM=pl.BlockSpec(memory_space=pltpu.VMEM)
def dot(a,b,dims=((1,),(0,))):
    return lax.dot_general(a,b,(dims,((),())),preferred_element_type=F32)
NT=((1,),(1,)); TN=((0,),(0,))
def norm_scale(wide): return lax.rsqrt(jnp.mean(wide*wide,-1,keepdims=True)+1e-6)
def normed(h):
    wide=h.astype(F32); return (wide*norm_scale(wide)).astype(BF)
def sigmoid(g): return 0.5*jnp.tanh(0.5*g)+0.5

def k1_body(x_ref,wg,wu,wd,gate_ref,up_ref,h_ref,a_ref,act,*,fc):
    x=x_ref[...]; a=normed(x); F=wg.shape[1]
    for c in range(F//fc):
        s=pl.ds(c*fc,fc)
        g=dot(a,wg[:,s]); u=dot(a,wu[:,s])
        gate_ref[:,s]=g; up_ref[:,s]=u
        act[:,s]=(g*sigmoid(g)*u).astype(BF)
    d=dot(act[...],wd[...]).astype(BF)
    h=(x.astype(F32)+d.astype(F32)).astype(BF)
    h_ref[...]=h; a_ref[...]=normed(h)
def k1(x,wg,wu,wd,bm=512,fc=768):
    T,D=x.shape; F=wg.shape[2]
    wspec=lambda r,c:pl.BlockSpec((None,r,c),lambda i:(0,0,0),pipeline_mode=pl.Buffered(1))
    row=lambda c:pl.BlockSpec((bm,c),lambda i:(i,0))
    return pl.pallas_call(functools.partial(k1_body,fc=fc),grid=(T//bm,),
        in_specs=[row(D),wspec(D,F),wspec(D,F),wspec(F,D)],
        out_specs=[row(F),row(F),row(D),row(D)],
        out_shape=[jax.ShapeDtypeStruct((T,F),F32)]*2+[jax.ShapeDtypeStruct((T,D),BF)]*2,
        scratch_shapes=[pltpu.VMEM((bm,F),BF)],
        compiler_params=pltpu.CompilerParams(vmem_limit_bytes=60<<20),name="k1",
        cost_estimate=pl.CostEstimate(flops=6*T*D*F,bytes_accessed=10*T*F,transcendentals=T*F))(x,wg,wu,wd)


MESH=pl.DeviceIdType.MESH
DMA=pltpu.SemaphoreType.DMA

class Shards:
    def __init__(s,n,D,F,ft):
        s.n=n; s.side=round((n//2)**0.5); s.D,s.F,s.ft=D,F,ft; s.nf=F//ft
        s.rg=D//n; s.rd=ft//n; s.nb=D//ft; s.rt=2*s.rg+s.rd*s.nb
        assert 2*s.side*s.side==n and s.rg*n==D and s.rd*n==ft and s.nb*ft==D

class Comm:
    NAMES=("loc","rc","f1","f2","fv","su1","su2","sv","own","P","sq","cS","cR","u1S","u1R","u2S","u2R","vS","vR","wS","wR","x1S","x1R","x2S","x2R","cgS","cgR","lS")
    @staticmethod
    def scratch(z,nl):
        S,nf,blk=z.side,z.nf,(z.rt,z.ft)
        V=lambda *s,dt=BF:pltpu.VMEM(s+blk,dt)
        h=S//2
        return [V(nl,2,S,S),V(nf,S,S),V(nf,2,h),V(nf,2,S),V(nf,S-1),V(2,S),V(2,2,S),V(2,S),V(2,dt=F32),V(nf,S),pltpu.VMEM(blk,F32),
            DMA((nf,)),DMA((nf,)),DMA((nf,2)),DMA((nf,2)),DMA((nf,2)),DMA((nf,2)),DMA((nf,S-1)),DMA((nf,S-1)),
            DMA((nf,S-1)),DMA((nf,S-1)),DMA((nf,2)),DMA((nf,2)),DMA((nf,2)),DMA((nf,2)),DMA((nf,)),DMA((nf,)),DMA((nf,))]
    STAGES=9
    def __init__(s,z,nl,refs,Q):
        s.z,s.nl,s.Q=z,nl,Q
        for nm,r in zip(s.NAMES,refs,strict=True): setattr(s,nm,r)
        me=lax.axis_index("dp"); S=z.side
        c=me%2; y=(me//2)%S; x=me//(2*S)
        s.me,s.c=me,c; s.u=x*(1-c)+y*c; s.v=y*(1-c)+x*c
        s.partner=me+1-2*c
        s.right=s.dev(s.u+1,s.v); s.left=s.dev(s.u+S-1,s.v)
        s.vpeer=[s.dev(s.u,s.v+d) for d in range(1,S)]
    def dev(s,u,v):
        S,c=s.z.side,s.c; u,v=u%S,v%S
        return ((u*(1-c)+v*c)*S+v*(1-c)+u*c)*2+c
    def greet(s,extra=()):
        b=pltpu.get_barrier_semaphore()
        for d in (s.partner,s.right,s.left,*s.vpeer,*extra): pl.semaphore_signal(b,inc=1,device_id={"dp":d},device_id_type=MESH)
    def met(s,extra=0):
        pl.semaphore_wait(pltpu.get_barrier_semaphore(),3+len(s.vpeer)+extra)
    def cp(s,src,dst,a,b,dev):
        return pltpu.make_async_remote_copy(src_ref=src,dst_ref=dst,send_sem=a,recv_sem=b,device_id={"dp":dev},device_id_type=MESH)
    def copies(s,i,k):
        S=s.z.side; h=S//2; n=lax.rem(k,s.nl); p=lax.rem(k,2); u,v,c=s.u,s.v,s.c
        ul,ur=(u+S-1)%S,(u+1)%S
        if i==0: return [s.cp(s.loc.at[n,1-c],s.rc.at[k],s.cS.at[k],s.cR.at[k],s.partner)]
        if i==1: return [s.cp(s.su1.at[p,pl.ds(0,h)],s.f1.at[k,0],s.u1S.at[k,0],s.u1R.at[k,0],s.right),
                         s.cp(s.su1.at[p,pl.ds(h,h)],s.f1.at[k,1],s.u1S.at[k,1],s.u1R.at[k,1],s.left)]
        if i==2: return [s.cp(s.su2.at[p,0],s.f2.at[k,0],s.u2S.at[k,0],s.u2R.at[k,0],s.right),
                         s.cp(s.su2.at[p,1],s.f2.at[k,1],s.u2S.at[k,1],s.u2R.at[k,1],s.left)]
        if i==3: return [s.cp(s.sv.at[p,(v+d)%S],s.fv.at[k,d-1],s.vS.at[k,d-1],s.vR.at[k,d-1],s.vpeer[d-1]) for d in range(1,S)]
        if i==4: return [s.cp(s.P.at[k,v],s.P.at[k,v],s.wS.at[k,d-1],s.wR.at[k,d-1],s.vpeer[d-1]) for d in range(1,S)]
        if i==5: return [s.cp(s.P.at[k],s.Q.at[c,k,u],s.x1S.at[k,0],s.x1R.at[k,0],s.right),
                         s.cp(s.P.at[k],s.Q.at[c,k,u],s.x1S.at[k,1],s.x1R.at[k,1],s.left)]
        if i==6: return [s.cp(s.Q.at[c,k,ul,pl.ds(0,h)],s.Q.at[c,k,ul,pl.ds(0,h)],s.x2S.at[k,0],s.x2R.at[k,0],s.right),
                         s.cp(s.Q.at[c,k,ur,pl.ds(h,h)],s.Q.at[c,k,ur,pl.ds(h,h)],s.x2S.at[k,1],s.x2R.at[k,1],s.left)]
        if i==7: return [s.cp(s.Q.at[c,k],s.Q.at[c,k],s.cgS.at[k],s.cgR.at[k],s.partner)]
    def arrived(s,i,k):
        S=s.z.side; h=S//2; u,v,c=s.u,s.v,s.c
        if i==4: return [s.cp(s.P.at[k,v],s.P.at[k,(v+S-d)%S],s.wS.at[k,d-1],s.wR.at[k,d-1],s.vpeer[d-1]) for d in range(1,S)]
        if i==5: return [s.cp(s.P.at[k],s.Q.at[c,k,(u+S-1)%S],s.x1S.at[k,0],s.x1R.at[k,0],s.right),
                         s.cp(s.P.at[k],s.Q.at[c,k,(u+1)%S],s.x1S.at[k,1],s.x1R.at[k,1],s.left)]
        if i==6:
            o=(u+h)%S
            return [s.cp(s.Q.at[c,k,o,pl.ds(0,h)],s.Q.at[c,k,o,pl.ds(0,h)],s.x2S.at[k,0],s.x2R.at[k,0],s.right),
                    s.cp(s.Q.at[c,k,o,pl.ds(h,h)],s.Q.at[c,k,o,pl.ds(h,h)],s.x2S.at[k,1],s.x2R.at[k,1],s.left)]
        if i==7: return [s.cp(s.Q.at[c,k],s.Q.at[1-c,k],s.cgS.at[k],s.cgR.at[k],s.partner)]
        return s.copies(i,k)
    def keep(s,k): return pltpu.make_async_copy(s.P.at[k],s.Q.at[s.c,k,s.u],s.lS.at[k])
    def stage(s,i,k):
        S=s.z.side; h=S//2; n=lax.rem(k,s.nl); p=lax.rem(k,2); u,v,c=s.u,s.v,s.c
        if i>0:
            for d in s.arrived(i-1,k): d.wait_recv()
            for d in s.copies(i-1,k): d.wait_send()
        f=lambda r:r[...].astype(F32)
        both=lambda q,sl:f(s.loc.at[n,c,q,sl])+f(s.rc.at[k,q,sl])
        A,B,al=pl.ds(0,h),pl.ds(h,h),pl.ds(0,S)
        if i==1:
            s.su1[p]=both((u+h)%S,al).astype(BF)
        if i==2:
            r,l=(u+1)%S,(u+S-1)%S
            s.su2[p,0,A]=(both(r,A)+f(s.f1.at[k,0])).astype(BF); s.su2[p,0,B]=both(r,B).astype(BF)
            s.su2[p,1,A]=both(l,A).astype(BF); s.su2[p,1,B]=(both(l,B)+f(s.f1.at[k,1])).astype(BF)
        if i==3:
            one=lambda r:f(s.loc.at[n,c,u,r])+f(s.rc.at[k,u,r])+f(s.f2.at[k,0,r])+f(s.f2.at[k,1,r])
            for d in range(1,S): s.sv[p,(v+d)%S]=one((v+d)%S).astype(BF)
            s.own[p]=one(v)
        if i==4:
            g=s.own[p]
            for d in range(S-1): g=g+f(s.fv.at[k,d])
            g=g.astype(BF); s.P[k,v]=g
            g=g.astype(F32); s.sq[...]+=g*g
        if i==5: s.keep(k).start()
        if i==7: s.keep(k).wait()
        if i<8:
            for d in s.copies(i,k): d.start()
    def point(s,stages,chunk):
        for i in stages:
            k=chunk(i)
            @pl.when((k>=0)&(k<s.z.nf))
            def _(i=i,k=k): s.stage(i,k)
    def store(s,k,a,part):
        z=s.z; S=z.side; n=lax.rem(k,s.nl)
        for i in range(z.n):
            at=(n,i//(S*S),i//S%S,i%S)
            if part<2: s.loc[(*at,pl.ds(part*z.rg,z.rg))]=a[i*z.rg:(i+1)*z.rg].astype(BF)
            else:
                for b in range(z.nb): s.loc[(*at,pl.ds(2*z.rg+b*z.rd,z.rd))]=a[i*z.rd:(i+1)*z.rd,b*z.ft:(b+1)*z.ft].astype(BF)

def elementwise(g,u,da):
    sg=sigmoid(g); silu=g*sg
    return (silu*u).astype(BF),(da*u*(sg+silu*(1.0-sg))).astype(BF),(da*silu).astype(BF)

def k2_body(a_ref,dy_ref,h_ref,wg_h,wu_h,wd_h,Q,ss_ref,dh_ref,wg,wu,wd,aT,dg,du,act,sem,*refs,z,nl,rc,bc,L):
    j=pl.program_id(0); T,D=a_ref.shape; nf,ft=z.nf,z.ft
    m=Comm(z,nl,refs,Q)
    def cps(t):
        s=pl.ds(pl.multiple_of(t*ft,ft),ft)
        return [pltpu.make_async_copy(wg_h.at[L,:,s],wg.at[:,s],sem.at[0,t]),pltpu.make_async_copy(wu_h.at[L,:,s],wu.at[:,s],sem.at[1,t]),
                pltpu.make_async_copy(wd_h.at[L,s,:],wd.at[lax.rem(t,2)],sem.at[2,t])]
    @pl.when(j==0)
    def _():
        m.greet()
        for c in cps(0): c.start()
        for t in range(1,nf):
            for c in cps(t)[:2]: c.start()
        m.sq[...]=jnp.zeros_like(m.sq)
        for r in range(0,T,rc): aT[:,pl.ds(r,rc)]=a_ref[pl.ds(r,rc),:].T
    s=pl.ds(pl.multiple_of(lax.rem(j,nf)*ft,ft),ft)
    @pl.when(j<nf)
    def _():
        for c in cps(j): c.wait()
        @pl.when(j+1<nf)
        def _(): cps(j+1)[2].start()
        wgt,wut,wdt=wg[:,s],wu[:,s],wd[lax.rem(j,2)]
        for r in range(0,T,rc):
            rs=pl.ds(r,rc); a=a_ref[rs,:]
            g=dot(a,wgt); u=dot(a,wut); da=dot(dy_ref[rs,:],wdt,NT).astype(BF).astype(F32)
            act[rs,:],dg[rs,s],du[rs,s]=elementwise(g,u,da)
    @pl.when(j==0)
    def _(): m.met()
    m.point((1,3,5,7),lambda i:(2*j-1-i)//2)
    @pl.when(j<nf)
    def _():
        m.store(j,dot(aT[...],dg[:,s]),0)
        m.store(j,dot(aT[...],du[:,s]),1)
        m.store(j,dot(act[...],dy_ref[...],TN),2)
    @pl.when(j>=nf)
    def _():
        rs=pl.ds(pl.multiple_of((j-nf)*bc,bc),bc)
        da=(dot(dg[rs,:],wg[...],NT).astype(BF).astype(F32)+dot(du[rs,:],wu[...],NT).astype(BF).astype(F32)).astype(BF).astype(F32)
        wide=h_ref[...].astype(F32); sc=norm_scale(wide)
        t=jnp.sum(da*wide,-1,keepdims=True)*(1.0/D)
        dn=(da*sc-wide*(sc*sc*sc*t)).astype(BF).astype(F32)
        dh_ref[...]=(dy_ref[rs,:].astype(F32)+dn).astype(BF)
    m.point((0,2,4,6,8),lambda i:(2*j-i)//2)
    @pl.when(j==pl.num_programs(0)-1)
    def _(): ss_ref[...]=m.sq[...]
def k2(a1,dy,h1,wg,wu,wd,n,L,ft=256,rc=512,bc=512):
    T,D=a1.shape; F=wg.shape[2]; z=Shards(n,D,F,ft); nf=z.nf; nb=T//bc; nl=2; S=z.side
    assert 2*(nf-1)+1+8<=2*(nf+nb)-1
    back=pl.BlockSpec((bc,D),lambda j:(jnp.maximum(j-nf,0),0))
    return pl.pallas_call(functools.partial(k2_body,z=z,nl=nl,rc=rc,bc=bc,L=L),grid=(nf+nb,),
        in_specs=[VM,VM,back,ANY,ANY,ANY],out_specs=[ANY,pl.BlockSpec((z.rt,ft),lambda j:(0,0)),back],
        out_shape=[jax.ShapeDtypeStruct((2,nf,S,S,z.rt,ft),BF),jax.ShapeDtypeStruct((z.rt,ft),F32),jax.ShapeDtypeStruct((T,D),BF)],
        scratch_shapes=[pltpu.VMEM((D,F),BF),pltpu.VMEM((D,F),BF),pltpu.VMEM((2,ft,D),BF),pltpu.VMEM((D,T),BF),
                        pltpu.VMEM((T,F),BF),pltpu.VMEM((T,F),BF),pltpu.VMEM((T,ft),BF),DMA((3,nf)),*Comm.scratch(z,nl)],
        compiler_params=pltpu.CompilerParams(vmem_limit_bytes=67043328,collective_id=1,has_side_effects=True),name="k2",
        cost_estimate=pl.CostEstimate(flops=16*T*D*F,bytes_accessed=30<<20,transcendentals=T*F))(a1,dy,h1,wg,wu,wd)

def k3_body(x_ref,dh_ref,g_ref,u_ref,wd_ref,ss_ref,Q,f_ref,aT,dg,du,act,nsend,nv,nu,nc,nS,nR,*refs,z,nl,rc,count):
    j=pl.program_id(0); T,D=x_ref.shape; nf,S=z.nf,z.side
    m=Comm(z,nl,refs,Q); last=nf-1+m.STAGES-1
    upeer=[m.dev(m.u+d,m.v) for d in range(1,S)]; far=[upeer[d] for d in range(1,S-2)]
    @pl.when(j==0)
    def _():
        m.greet(far)
        m.sq[...]=ss_ref[...]
        for r in range(0,T,rc): aT[:,pl.ds(r,rc)]=normed(x_ref[pl.ds(r,rc),:]).T
    @pl.when(j<nf)
    def _():
        wdt=wd_ref[...]
        for r in range(0,T,rc):
            rs=pl.ds(r,rc)
            da=dot(dh_ref[rs,:],wdt,NT).astype(BF).astype(F32)
            act[rs,:],dg[rs,:],du[rs,:]=elementwise(g_ref[rs,:],u_ref[rs,:],da)
        m.store(j,dot(aT[...],dg[...]),0)
        m.store(j,dot(aT[...],du[...]),1)
        m.store(j,dot(act[...],dh_ref[...],TN),2)
    @pl.when(j==0)
    def _(): m.met(len(far))
    m.point(range(9),lambda i:j-i)
    def cps(buf,at,peers,b): return [m.cp(nsend.at[b],buf.at[at],nS.at[b,i],nR.at[b,i],p) for i,p in enumerate(peers)]
    def wait(buf,at,peers,b):
        for i in range(len(peers)):
            m.cp(nsend.at[b],buf.at[at[i]],nS.at[b,i],nR.at[b,i],peers[i]).wait()
    def total(ref,k):
        t=ref[0]
        for i in range(1,k): t=t+ref[i]
        return t
    @pl.when(j==last-3)
    def _():
        t=jnp.broadcast_to(jnp.sum(jnp.sum(m.sq[...],0,keepdims=True),1,keepdims=True),(8,128))
        nsend[0]=t; nv[m.v]=t
        for d in cps(nv,m.v,m.vpeer,0): d.start()
    @pl.when(j==last-2)
    def _():
        wait(nv,[(m.v+S-d)%S for d in range(1,S)],m.vpeer,0)
        t=total(nv,S); nsend[1]=t; nu[m.u]=t
        for d in cps(nu,m.u,upeer,1): d.start()
    @pl.when(j==last-1)
    def _():
        wait(nu,[(m.u+S-d)%S for d in range(1,S)],upeer,1)
        t=total(nu,S); nsend[2]=t; nc[m.c]=t
        for d in cps(nc,m.c,[m.partner],2): d.start()
    @pl.when(j==last)
    def _():
        wait(nc,[1-m.c],[m.partner],2)
        f_ref[...]=jnp.minimum(1.0,0.5*lax.rsqrt(total(nc,2)*(1.0/count)+1e-30))
def k3(x,dh,gate,up,wd,ss,n,L,count,ft=256,rc=512):
    T,D=x.shape; F=gate.shape[1]; z=Shards(n,D,F,ft); nf=z.nf; S=z.side; nl=4
    cl=lambda j:jnp.minimum(j,nf-1)
    col=lambda r:pl.BlockSpec((r,ft),lambda j:(0,cl(j)))
    return pl.pallas_call(functools.partial(k3_body,z=z,nl=nl,rc=rc,count=count),grid=(nf+Comm.STAGES-1,),
        in_specs=[VM,VM,col(T),col(T),pl.BlockSpec((None,ft,D),lambda j:(L,cl(j),0)),VM],
        out_specs=[ANY,pl.BlockSpec((8,128),lambda j:(0,0))],
        out_shape=[jax.ShapeDtypeStruct((2,nf,S,S,z.rt,ft),BF),jax.ShapeDtypeStruct((8,128),F32)],
        scratch_shapes=[pltpu.VMEM((D,T),BF)]+[pltpu.VMEM((T,ft),BF)]*3+[pltpu.VMEM((3,8,128),F32),pltpu.VMEM((S,8,128),F32),pltpu.VMEM((S,8,128),F32),
            pltpu.VMEM((2,8,128),F32),DMA((3,S-1)),DMA((3,S-1)),*Comm.scratch(z,nl)],
        compiler_params=pltpu.CompilerParams(vmem_limit_bytes=67043328,collective_id=2,has_side_effects=True),name="k3",
        cost_estimate=pl.CostEstimate(flops=8*T*D*F,bytes_accessed=10*T*F,transcendentals=T*F))(x,dh,gate,up,wd,ss)

def adam_body(f_ref,g1,g0,*refs,z,half):
    ins,outs=refs[:9],refs[9:]
    i=pl.program_id(0); S,ft,rg,rd,nb=z.side,z.ft,z.rg,z.rd,z.nb
    f=f_ref[0:1,0:1]
    def one(g,w,m,v,wo,mo,vo,at):
        g=g.astype(F32)*f
        m=0.9*m[at]+0.1*g
        v=0.95*v[at]+0.05*g*g
        w=w[at].astype(F32)
        wo[at]=(w-0.02*(m*lax.rsqrt(v+1e-8)+0.1*w)).astype(BF); mo[at]=m; vo[at]=v
    def piece(q):
        def tile(t,_):
            cs=pl.ds(pl.multiple_of(t*ft,ft),ft)
            for r in range(S):
                for a in range(2):
                    one(q[t,r,pl.ds(a*rg,rg),:],*(ins[a+3*b] for b in range(3)),*(outs[a+3*b] for b in range(3)),(pl.ds(r*rg,rg),cs))
                for b in range(nb):
                    one(q[t,r,pl.ds(2*rg+b*rd,rd),:],*(ins[2+3*b_] for b_ in range(3)),*(outs[2+3*b_] for b_ in range(3)),(t,pl.ds(r*rd,rd),pl.ds(b*ft,ft)))
            return _
        lax.fori_loop(0,z.nf,tile,0)
    @pl.when(i<half)
    def _(): piece(g1)
    @pl.when(i>=half)
    def _(): piece(g0)
def adam(f,G1,G0,w,m,v,n,ft=256):
    L,D,F=w[0].shape; z=Shards(n,D,F,ft); S,nf=z.side,z.nf; hf=2*S; rows=D//hf
    one=lambda a:a.reshape(L*hf,rows,F)
    dn=lambda a:a.reshape(L,nf,hf,ft//hf,D)
    args=[(dn if k==2 else one)(a) for t in (w,m,v) for k,a in enumerate(t)]
    lay=lambda i:1-i//hf
    bo=pl.BlockSpec((None,rows,F),lambda i:(lay(i)*hf+i%hf,0,0)); bd=pl.BlockSpec((None,nf,None,ft//hf,D),lambda i:(lay(i),0,i%hf,0,0))
    g1=lambda i:(jnp.minimum(i,hf-1)); g0=lambda i:jnp.maximum(i-hf,0)
    gs=lambda k:pl.BlockSpec((None,nf,None,S,z.rt,ft),lambda i:(k(i)//S,0,k(i)%S,0,0,0))
    specs=[bo,bo,bd]*3
    out=pl.pallas_call(functools.partial(adam_body,z=z,half=hf),grid=(L*hf,),
        in_specs=[pl.BlockSpec((8,128),lambda i:(0,0)),gs(g1),gs(g0)]+specs,out_specs=specs,
        out_shape=[jax.ShapeDtypeStruct(a.shape,a.dtype) for a in args],
        compiler_params=pltpu.CompilerParams(vmem_limit_bytes=56<<20),name="adamw",
        cost_estimate=pl.CostEstimate(flops=60*L*D*F,bytes_accessed=66*L*D*F,transcendentals=3*L*D*F))(f,G1,G0,*args)
    return [o.reshape(a.shape) for o,a in zip(out,[*w,*m,*v])]

def solution(mesh):
    n=mesh.shape["dp"]
    def step(x,dy,*arrays):
        w,m,v=(arrays[i:i+3] for i in (0,3,6))
        count=sum(a.size for a in w)
        gate,up,h1,a1=k1(x[0],*w)
        G1,ss,dh=k2(a1,dy[0],h1,*w,n,1)
        G0,f=k3(x[0],dh,gate,up,w[2],ss,n,0,count)
        return tuple(adam(f,G1,G0,w,m,v,n))
    return jax.shard_map(step,mesh=mesh,in_specs=(P(("rep","dp"),None,None),)*2+(P(None,None,None),)*9,
        out_specs=(P("rep",None,None),)*9,check_vma=False)
```

```python
import functools
import jax, jax.numpy as jnp
from jax import lax
from jax.experimental import pallas as pl
from jax.experimental.pallas import tpu as pltpu
from jax.sharding import PartitionSpec
F32,BF=jnp.float32,jnp.bfloat16
ANY=pl.BlockSpec(memory_space=pl.ANY)
VM=pl.BlockSpec(memory_space=pltpu.VMEM)
def dot(a,b,dims=((1,),(0,))):
    return lax.dot_general(a,b,(dims,((),())),preferred_element_type=F32)
NT=((1,),(1,)); TN=((0,),(0,))
def norm_scale(wide): return lax.rsqrt(jnp.mean(wide*wide,-1,keepdims=True)+1e-6)
def normed(h):
    wide=h.astype(F32); return (wide*norm_scale(wide)).astype(BF)
def sigmoid(g): return 0.5*jnp.tanh(0.5*g)+0.5

def k1_body(x_ref,wg,wu,wd,gate_ref,up_ref,h_ref,a_ref,aT_ref,act,*,fc):
    x=x_ref[...]; a=normed(x); F=wg.shape[1]; aT_ref[...]=a.T
    for c in range(F//fc):
        s=pl.ds(c*fc,fc)
        g=dot(a,wg[:,s]); u=dot(a,wu[:,s])
        gate_ref[:,s]=g; up_ref[:,s]=u
        act[:,s]=(g*sigmoid(g)*u).astype(BF)
    d=dot(act[...],wd[...]).astype(BF)
    h=(x.astype(F32)+d.astype(F32)).astype(BF)
    h_ref[...]=h; a_ref[...]=normed(h)
def k1(x,wg,wu,wd,bm=512,fc=768):
    T,D=x.shape; F=wg.shape[2]
    wspec=lambda r,c:pl.BlockSpec((None,r,c),lambda i:(0,0,0),pipeline_mode=pl.Buffered(1))
    row=lambda c:pl.BlockSpec((bm,c),lambda i:(i,0))
    return pl.pallas_call(functools.partial(k1_body,fc=fc),grid=(T//bm,),
        in_specs=[row(D),wspec(D,F),wspec(D,F),wspec(F,D)],
        out_specs=[row(F),row(F),row(D),row(D),pl.BlockSpec((D,bm),lambda i:(0,i))],
        out_shape=[jax.ShapeDtypeStruct((T,F),F32)]*2+[jax.ShapeDtypeStruct((T,D),BF)]*2+[jax.ShapeDtypeStruct((D,T),BF)],
        scratch_shapes=[pltpu.VMEM((bm,F),BF)],
        compiler_params=pltpu.CompilerParams(vmem_limit_bytes=60<<20),name="k1",
        cost_estimate=pl.CostEstimate(flops=6*T*D*F,bytes_accessed=10*T*F,transcendentals=T*F))(x,wg,wu,wd)


MESH=pl.DeviceIdType.MESH
DMA=pltpu.SemaphoreType.DMA
LANES=128

class Shards:
    def __init__(s,n,D,F,ft):
        s.n=n; s.side=round((n//2)**0.5); s.D,s.F,s.ft=D,F,ft; s.nf=F//ft
        s.rg=D//n; s.rd=ft//n; s.part=s.rg*ft//LANES; s.blk=(3*s.part,LANES)
        assert 2*s.side*s.side==n and s.rg*n==D and s.rd*n==ft and ft%LANES==0 and D%LANES==0

class Place:
    def __init__(s,S):
        me=lax.axis_index("dp"); c=me%2; y=(me//2)%S; x=me//(2*S)
        s.S,s.c,s.u,s.v=S,c,x*(1-c)+y*c,y*(1-c)+x*c
        s.partner=me+1-2*c; s.right=s.dev(s.u+1,s.v); s.left=s.dev(s.u+S-1,s.v)
        s.vpeer=[s.dev(s.u,s.v+d) for d in range(1,S)]; s.upeer=[s.dev(s.u+d,s.v) for d in range(1,S)]
    def place(s,layer,other,d):
        S,c=s.S,s.c; return (layer*2+(1-c if other else c))*S+((s.v if other else s.u)+S-d)%S
    def dev(s,u,v):
        S,c=s.S,s.c; u,v=u%S,v%S
        return ((u*(1-c)+v*c)*S+v*(1-c)+u*c)*2+c
    def greet(s,peers):
        b=pltpu.get_barrier_semaphore()
        for d in peers: pl.semaphore_signal(b,inc=1,device_id={"dp":d},device_id_type=MESH)

def send(src,dst,a,b,dev):
    return pltpu.make_async_remote_copy(src_ref=src,dst_ref=dst,send_sem=a,recv_sem=b,device_id={"dp":dev},device_id_type=MESH)
def wide(r): return r[...].astype(F32)

class Scatter:
    N=13
    @staticmethod
    def scratch(z,nl,ns):
        S,nf,blk=z.side,z.nf,z.blk
        V=lambda *s,dt=BF:pltpu.VMEM(s+blk,dt)
        return [V(nl,2,S,S),V(nf,S,S),V(nf,S-1,S),V(nf,S-1),V(ns,S-1,S),V(ns,S-1),V(ns,dt=F32),DMA((nf,)),DMA((nf,)),*[DMA((nf,S-1))]*4]
    def __init__(s,z,pos,nl,ns,refs):
        s.z,s.pos,s.nl,s.ns=z,pos,nl,ns
        (s.loc,s.rc,s.fu,s.fv,s.su,s.sv,s.own,s.cS,s.cR,s.uS,s.uR,s.vS,s.vR)=refs
    def copies(s,i,k):
        o=s.pos; n=lax.rem(k,s.nl); p=lax.rem(k,s.ns)
        if i==0: return [send(s.loc.at[n,1-o.c],s.rc.at[k],s.cS.at[k],s.cR.at[k],o.partner)]
        if i==1: return [send(s.su.at[p,d],s.fu.at[k,d],s.uS.at[k,d],s.uR.at[k,d],to) for d,to in enumerate(o.upeer)]
        if i==2: return [send(s.sv.at[p,d],s.fv.at[k,d],s.vS.at[k,d],s.vR.at[k,d],to) for d,to in enumerate(o.vpeer)]
    def step(s,i,k,done=None):
        o=s.pos; S=o.S; n=lax.rem(k,s.nl); p=lax.rem(k,s.ns); u,v,c=o.u,o.v,o.c
        if i>0:
            for d in s.copies(i-1,k): d.wait()
        both=lambda q,sl:wide(s.loc.at[n,c,q,sl])+wide(s.rc.at[k,q,sl])
        if i==1:
            for d in range(S-1): s.su[p,d]=both((u+d+1)%S,pl.ds(0,S)).astype(BF)
        if i==2:
            def one(r):
                t=both(u,r)
                for d in range(S-1): t=t+wide(s.fu.at[k,d,r])
                return t
            for d in range(S-1): s.sv[p,d]=one((v+d+1)%S).astype(BF)
            s.own[p]=one(v)
        if i==3:
            g=s.own[p]
            for d in range(S-1): g=g+wide(s.fv.at[k,d])
            done(k,g.astype(BF))
        if i<3:
            for d in s.copies(i,k): d.start()
    def store(s,k,a,part):
        z=s.z; S=z.side; n=lax.rem(k,s.nl); r=z.rd if part==2 else z.rg
        for i in range(z.n):
            rows=a[i*r:(i+1)*r]
            s.loc[n,i//(S*S),i//S%S,i%S,pl.ds(part*z.part,z.part)]=jnp.concatenate([rows[:,b:b+LANES] for b in range(0,a.shape[1],LANES)],0).astype(BF)

class Gather:
    N=10
    @staticmethod
    def scratch(z,count):
        S=z.side
        return [pltpu.VMEM((count,S,*z.blk),BF),*[DMA((count,S-1))]*2,*[DMA((count,2))]*4,*[DMA((count,))]*3]
    def __init__(s,z,pos,first,Q,refs):
        s.z,s.pos,s.first,s.Q=z,pos,first,Q
        (s.P,s.wS,s.wR,s.aS,s.aR,s.bS,s.bR,s.cS,s.cR,s.lS)=refs
    def copies(s,i,k,here=False):
        o=s.pos; S=o.S; h=S//2; u,v,c=o.u,o.v,o.c; q=k+s.first; l,r=(u+S-1)%S,(u+1)%S; P,Q=s.P,s.Q
        A,B=pl.ds(0,h),pl.ds(h,h)
        if i==0: return [send(P.at[k,v],P.at[k,(v+S-d)%S if here else v],s.wS.at[k,d-1],s.wR.at[k,d-1],o.vpeer[d-1]) for d in range(1,S)]
        if i==1: return [send(P.at[k],Q.at[c,q,(l,r)[w] if here else u],s.aS.at[k,w],s.aR.at[k,w],d) for w,d in enumerate((o.right,o.left))]
        if i==2: return [send(Q.at[c,q,(l,r)[w],(A,B)[w]],Q.at[c,q,(u+h)%S if here else (l,r)[w],(A,B)[w]],s.bS.at[k,w],s.bR.at[k,w],d) for w,d in enumerate((o.right,o.left))]
        if i==3: return [send(Q.at[c,q],Q.at[1-c if here else c,q],s.cS.at[k],s.cR.at[k],o.partner)]
    def keep(s,k): return pltpu.make_async_copy(s.P.at[k],s.Q.at[s.pos.c,k+s.first,s.pos.u],s.lS.at[k])
    def step(s,i,k):
        if i>0:
            for d in s.copies(i-1,k,True): d.wait()
        if i==1: s.keep(k).start()
        if i==3: s.keep(k).wait()
        if i<4:
            for d in s.copies(i,k): d.start()

def run(points,p,parity,do):
    if not any(t%2==parity for t in points): return
    upto=lambda q:sum((q>=t).astype(jnp.int32) for t in points)
    lax.fori_loop(upto(p-1),upto(p),lambda k,_:(do(k),0)[1],0)

def elementwise(g,u,da):
    sg=sigmoid(g); silu=g*sg
    return (silu*u).astype(BF),(da*u*(sg+silu*(1.0-sg))).astype(BF),(da*silu).astype(BF)

def check_points(rs,nl,ns,later):
    nf=len(rs)
    for k in range(nf):
        assert rs[k][0]==2*(k+later)+1 and all(a<b for a,b in zip(rs[k],rs[k][1:])),rs[k]
        if k>=nl: assert rs[k-nl][2]<2*(k+later)
        if k>=ns: assert all(rs[k-ns][i+1]<=rs[k][i] for i in (1,2))
        if k: assert all(a<=b for a,b in zip(rs[k-1],rs[k]))
def check_gather(ag,starts=None):
    for k,t in enumerate(ag):
        assert all(a<b for a,b in zip(t,t[1:])) and (not starts or t[0]==starts[k]),t
        if k: assert all(a<=b for a,b in zip(ag[k-1],t))

def k2_body(a_ref,dy_ref,h_ref,wg_h,wu_h,wd_h,Q,ss_ref,left_ref,dh_ref,wg,wu,wd,aT,dg,du,act,sem,*refs,z,nl,ns,rc,bc,L,rs,ag):
    j=pl.program_id(0); T,D=a_ref.shape; nf,ft=z.nf,z.ft; na=len(ag); nb=T//bc
    o=Place(z.side); sc=Scatter(z,o,nl,ns,refs[:Scatter.N]); ga=Gather(z,o,0,Q,refs[Scatter.N:])
    def done(k,g):
        w=g.astype(F32); ss_ref[...]+=w*w
        @pl.when(k<na)
        def _(): ga.P[k,o.v]=g; ga.step(0,k)
        if na<nf:
            @pl.when(k>=na)
            def _(): left_ref[k-na]=g
    def point(p,parity):
        for i in (3,2,1,0): run([t[i] for t in rs],p,parity,lambda k:sc.step(i,k,done))
        for i in (4,3,2,1): run([t[i] for t in ag],p,parity,lambda k:ga.step(i,k))
    def cps(t):
        s=pl.ds(pl.multiple_of(t*ft,ft),ft)
        return [pltpu.make_async_copy(wg_h.at[L,:,s],wg.at[:,s],sem.at[0,t]),pltpu.make_async_copy(wu_h.at[L,:,s],wu.at[:,s],sem.at[1,t]),
                pltpu.make_async_copy(wd_h.at[L,s,:],wd.at[lax.rem(t,2)],sem.at[2,t])]
    @pl.when(j==0)
    def _():
        o.greet((o.partner,*o.upeer,*o.vpeer))
        for c in cps(0): c.start()
        for t in range(1,nf):
            for c in cps(t)[:2]: c.start()
        ss_ref[...]=jnp.zeros_like(ss_ref)
        for r in range(0,T,rc): aT[:,pl.ds(r,rc)]=a_ref[pl.ds(r,rc),:].T
    s=pl.ds(pl.multiple_of(lax.rem(j,nf)*ft,ft),ft)
    @pl.when(j<nf)
    def _():
        for c in cps(j): c.wait()
        @pl.when(j+1<nf)
        def _(): cps(j+1)[2].start()
        wgt,wut,wdt=wg[:,s],wu[:,s],wd[lax.rem(j,2)]
        for r in range(0,T,rc):
            rs_=pl.ds(r,rc); a=a_ref[rs_,:]
            g=dot(a,wgt); u=dot(a,wut); da=dot(dy_ref[rs_,:],wdt,NT).astype(BF).astype(F32)
            act[rs_,:],dg[rs_,s],du[rs_,s]=elementwise(g,u,da)
    @pl.when(j==0)
    def _(): pl.semaphore_wait(pltpu.get_barrier_semaphore(),1+len(o.upeer)+len(o.vpeer))
    point(2*j,0)
    @pl.when(j<nf)
    def _():
        sc.store(j,dot(aT[...],dg[:,s]),0)
        sc.store(j,dot(aT[...],du[:,s]),1)
        sc.store(j,dot(act[...],dy_ref[...],TN),2)
    @pl.when((j>=nf)&(j<nf+nb))
    def _():
        rs_=pl.ds(pl.multiple_of((j-nf)*bc,bc),bc)
        da=(dot(dg[rs_,:],wg[...],NT).astype(BF).astype(F32)+dot(du[rs_,:],wu[...],NT).astype(BF).astype(F32)).astype(BF).astype(F32)
        x=h_ref[...].astype(F32); scale=norm_scale(x)
        t=jnp.sum(da*x,-1,keepdims=True)*(1.0/D)
        dn=(da*scale-x*(scale*scale*scale*t)).astype(BF).astype(F32)
        dh_ref[...]=(dy_ref[rs_,:].astype(F32)+dn).astype(BF)
    point(2*j+1,1)
def k2(a1,dy,h1,wg,wu,wd,n,L,points,ft=256,rc=512,bc=256,nl=4,ns=3):
    T,D=a1.shape; F=wg.shape[2]; z=Shards(n,D,F,ft); nf=z.nf; nb=T//bc; S=z.side
    rs,ag=points; steps=max(nf+nb,max(t[-1] for t in rs+ag)//2+1); check_points(rs,nl,ns,0); check_gather(ag,[t[3] for t in rs]); nleft=max(nf-len(ag),1)
    back=pl.BlockSpec((bc,D),lambda j:(jnp.clip(j-nf,0,nb-1),0)); all_=lambda *s:pl.BlockSpec(s,lambda j:(0,)*len(s))
    return pl.pallas_call(functools.partial(k2_body,z=z,nl=nl,ns=ns,rc=rc,bc=bc,L=L,rs=rs,ag=ag),grid=(steps,),
        in_specs=[VM,VM,back,ANY,ANY,ANY],out_specs=[ANY,all_(*z.blk),all_(nleft,*z.blk),back],
        out_shape=[jax.ShapeDtypeStruct((2,nf,S,S,*z.blk),BF),jax.ShapeDtypeStruct(z.blk,F32),jax.ShapeDtypeStruct((nleft,*z.blk),BF),jax.ShapeDtypeStruct((T,D),BF)],
        scratch_shapes=[pltpu.VMEM((D,F),BF),pltpu.VMEM((D,F),BF),pltpu.VMEM((2,ft,D),BF),pltpu.VMEM((D,T),BF),
                        pltpu.VMEM((T,F),BF),pltpu.VMEM((T,F),BF),pltpu.VMEM((T,ft),BF),DMA((3,nf)),*Scatter.scratch(z,nl,ns),*Gather.scratch(z,max(len(ag),1))],
        compiler_params=pltpu.CompilerParams(vmem_limit_bytes=67043328,collective_id=1,has_side_effects=True),name="k2",
        cost_estimate=pl.CostEstimate(flops=16*T*D*F,bytes_accessed=30<<20,transcendentals=T*F))(a1,dy,h1,wg,wu,wd)

def k3_body(aT_h,dh_ref,g_ref,u_ref,wd_ref,ss_ref,left_ref,Q1_,P_out,f_ref,Q1,P_ref,aT,dg,du,act,sq,nsend,nv,nu,nc,nS,nR,gS,gR,oS,sem,*refs,z,nl,ns,rc,count,rs,ag,left,sqp):
    j=pl.program_id(0); D,T=aT.shape; nf,S=z.nf,z.side
    o=Place(S); sc=Scatter(z,o,nl,ns,refs[:Scatter.N])
    nleft=len(left); gl=Gather(z,o,nf-nleft,Q1,refs[Scatter.N:]) if nleft else None
    to=lambda k,here=False:[send(P_ref.at[k,o.v],P_ref.at[k,(o.v+S-d)%S if here else o.v],gS.at[k,d-1],gR.at[k,d-1],o.vpeer[d-1]) for d in range(1,S)]
    def done(k,g):
        w=g.astype(F32); sq[...]+=w*w
        P_ref[k,o.v]=g
        for d in to(k): d.start()
    def there(k):
        for d in to(k,True): d.wait()
        give(k).start()
    give=lambda k:pltpu.make_async_copy(P_ref.at[k],P_out.at[k],oS.at[k])
    def reduce_(p,parity):
        for i in (3,2,1,0): run([t[i] for t in rs],p,parity,lambda k:sc.step(i,k,done))
    def rest(p,parity):
        if nleft:
            for i in (4,3,2,1,0): run([t[i] for t in left],p,parity,lambda k:gl.step(i,k))
        run([t[1] for t in ag],p,parity,there)
    load=pltpu.make_async_copy(aT_h,aT,sem)
    def front(rows,b):
        for r in rows:
            rs_=pl.ds(r,rc)
            da=dot(dh_ref[rs_,:],wd_ref[...],NT).astype(BF).astype(F32)
            act[b,rs_,:],dg[b,rs_,:],du[b,rs_,:]=elementwise(g_ref[rs_,:],u_ref[rs_,:],da)
    def back(k,part,b):
        if part<2: sc.store(k,dot(aT[...],(dg,du)[part][b]),part)
        else: sc.store(k,dot(act[b],dh_ref[...],TN),2)
    rows=range(0,T,rc); half=len(rows)//2; b=lax.rem(j,2)
    @pl.when(j==0)
    def _():
        load.start()
        o.greet((o.partner,*o.upeer,*o.vpeer))
        sq[...]=ss_ref[...]
        for k in range(nleft): gl.P[k,o.v]=left_ref[k]
        front(rows[:half],b)
    @pl.when((j>0)&(j<nf))
    def _():
        front(rows[:half],b); back(j-1,0,1-b)
    @pl.when(j==nf)
    def _(): back(j-1,0,1-b)
    @pl.when(j==0)
    def _(): pl.semaphore_wait(pltpu.get_barrier_semaphore(),1+len(o.upeer)+len(o.vpeer))
    reduce_(2*j,0); rest(2*j,0)
    @pl.when(j==0)
    def _():
        front(rows[half:],b); load.wait()
    @pl.when((j>0)&(j<nf))
    def _():
        back(j-1,1,1-b); front(rows[half:],b); back(j-1,2,1-b)
    @pl.when(j==nf)
    def _(): back(j-1,1,1-b); back(j-1,2,1-b)
    p=2*j+1
    reduce_(p,1)
    def sums(buf,at,peers,b): return [send(nsend.at[b],buf.at[a],nS.at[b,i],nR.at[b,i],d) for i,(a,d) in enumerate(zip(at,peers))]
    def total(ref,k):
        t=ref[0]
        for i in range(1,k): t=t+ref[i]
        return t
    hops=((nv,o.v,o.vpeer,[(o.v+S-d)%S for d in range(1,S)],S),(nu,o.u,o.upeer,[(o.u+S-d)%S for d in range(1,S)],S),(nc,o.c,[o.partner],[1-o.c],2))
    for b_ in range(4):
        @pl.when(p==sqp[b_])
        def _(b=b_):
            if b==0: t=jnp.broadcast_to(jnp.sum(jnp.sum(sq[...],0,keepdims=True),1,keepdims=True),(8,128))
            else:
                buf,_,peers,at,k=hops[b-1]
                for d in sums(buf,at,peers,b-1): d.wait()
                t=total(buf,k)
            if b<3:
                buf,mine,peers,_,_=hops[b]
                nsend[b]=t; buf[mine]=t
                for d in sums(buf,[mine]*len(peers),peers,b): d.start()
            else: f_ref[...]=jnp.minimum(1.0,0.5*lax.rsqrt(t*(1.0/count)+1e-30))
    rest(p,1)
    @pl.when(j==pl.num_programs(0)-1)
    def _():
        for k in range(nf): give(k).wait()
def k3(a0T,dh,gate,up,wd,ss,left,Q1,n,L,count,points,ft=256,rc=512,nl=6,ns=4,nleft=2):
    D,T=a0T.shape; F=gate.shape[1]; z=Shards(n,D,F,ft); nf=z.nf; S=z.side
    rs,ag,lp,sqp=points; steps=max(max(t[-1] for t in rs+ag+lp),sqp[-1])//2+1
    assert len(lp)==nleft
    check_points(rs,nl,ns,1); check_gather(ag,[t[3] for t in rs]); check_gather(lp)
    cl=lambda j:jnp.minimum(j,nf-1); all_=lambda *s:pl.BlockSpec(s,lambda j:(0,)*len(s))
    col=lambda r:pl.BlockSpec((r,ft),lambda j:(0,cl(j)))
    return pl.pallas_call(functools.partial(k3_body,z=z,nl=nl,ns=ns,rc=rc,count=count,rs=rs,ag=ag,left=lp,sqp=sqp),grid=(steps,),
        in_specs=[ANY,VM,col(T),col(T),pl.BlockSpec((None,ft,D),lambda j:(L,cl(j),0)),VM,VM,ANY],
        out_specs=[ANY,all_(8,128),ANY],
        out_shape=[jax.ShapeDtypeStruct((nf,S,*z.blk),BF),jax.ShapeDtypeStruct((8,128),F32),jax.ShapeDtypeStruct(Q1.shape,BF)],input_output_aliases={7:2},
        scratch_shapes=[pltpu.VMEM((nf,S,*z.blk),BF),pltpu.VMEM((D,T),BF)]+[pltpu.VMEM((2,T,ft),BF)]*3+[pltpu.VMEM(z.blk,F32),pltpu.VMEM((3,8,128),F32),pltpu.VMEM((S,8,128),F32),pltpu.VMEM((S,8,128),F32),
            pltpu.VMEM((2,8,128),F32),DMA((3,S-1)),DMA((3,S-1)),DMA((nf,S-1)),DMA((nf,S-1)),DMA((nf,)),DMA,*Scatter.scratch(z,nl,ns),*(Gather.scratch(z,nleft) if nleft else [])],
        compiler_params=pltpu.CompilerParams(vmem_limit_bytes=67043328,collective_id=2,has_side_effects=True),name="k3",
        cost_estimate=pl.CostEstimate(flops=8*T*D*F,bytes_accessed=10*T*F,transcendentals=T*F))(a0T,dh,gate,up,wd,ss,left,Q1)


def points(rows):
    return [[ord(c) - ord("0") for c in row] for row in rows.split(",")]


K2_POINTS = (points("1257,3479,569;,78;=,9:=?,;<?A,=>AG,?@EM,ACKO"), points("79=?A,9;?AE,;=AGK,=?EMQ,?AIMQ"))
K3_POINTS = (points("359<,57;>,79=@,9;?B,;=AI,=?GS,?AMY,AEQ[,CKW_"), points("<?,>A,@I,BO,IU,S],Ya,[c,_g"), points("0369;,048;=,04:=?,06<?A"), points("_eik")[0])

def adam_body(f_ref,*refs,z,plan,ng,alias,sub,depth):
    gs,refs=refs[:ng],refs[ng:]; ins=refs[:9]; outs=refs[9+alias:18+alias]
    gb,refs=refs[18+alias],refs[19+alias:]; ib,ob,(isem,osem)=refs[:9],refs[9:18],refs[18:]
    S,ft,rg,rd,nf=z.side,z.ft,z.rg,z.rd,z.nf; rs=S//sub; hf=2*S; N=len(plan)*sub
    f=f_ref[0:1,0:1]; o=Place(S)
    places=[(l*2+h)*S+part if h is not None else o.place(l,*part) for l,h,part,_ in plan]
    def at(ref,q,t):
        p=sum(jnp.where(t//sub==k,place,0) for k,place in enumerate(places)); h=lax.rem(t,sub)
        if q%3<2: return ref.at[p,pl.ds(pl.multiple_of(h*(rs*rg),8),rs*rg)]
        return ref.at[p//hf,:,lax.rem(p,hf),pl.ds(pl.multiple_of(h*(rs*rd),8),rs*rd)]
    def reads(t):
        b=lax.rem(t,depth); return [pltpu.make_async_copy(at(ins[q],q,t),ib[q].at[b],isem.at[b,q]) for q in range(9)]
    def writes(t):
        b=lax.rem(t,depth); return [pltpu.make_async_copy(ob[q].at[b],at(outs[q],q,t),osem.at[b,q]) for q in range(9)]
    def gread(ref,part,t):
        b=lax.rem(t,depth); h=lax.rem(t,sub)
        src=(ref if part is None else ref.at[part[0],:,part[1]]).at[:,pl.ds(h*rs,rs)]
        return pltpu.make_async_copy(src,gb.at[b],isem.at[b,9])
    def fetch(t):
        for c in reads(t): c.start()
        for k,(_,h,part,a) in enumerate(plan):
            @pl.when(t//sub==k)
            def _(a=a,part=None if h is None else (h,part)): gread(gs[a],part,t).start()
    def one(g,w,m,v,wo,mo,vo,at):
        g=g.astype(F32)*f
        m=0.9*m[at]+0.1*g
        v=0.95*v[at]+0.05*g*g
        w=w[at].astype(F32)
        wo[at]=(w-0.02*(m*lax.rsqrt(v+1e-8)+0.1*w)).astype(BF); mo[at]=m; vo[at]=v
    for t in range(depth-1): fetch(jnp.int32(t))
    def unit(t,_):
        b=lax.rem(t,depth)
        @pl.when(t+depth-1<N)
        def _(): fetch(t+depth-1)
        for c in reads(t): c.wait()
        pltpu.make_async_copy(gb.at[b],gb.at[b],isem.at[b,9]).wait()
        @pl.when(t>=depth)
        def _():
            for c in writes(t-depth): c.wait()
        def tile(k,_):
            for r in range(rs):
                for q in range(3):
                    rows,cols=(rd,z.D) if q==2 else (rg,ft)
                    for c in range(0,cols,LANES):
                        g=gb[b,k,r,pl.ds(q*z.part+c//LANES*rows,rows),:]
                        at=(k,pl.ds(r*rows,rows),pl.ds(c,LANES)) if q==2 else (pl.ds(r*rows,rows),pl.ds(pl.multiple_of(k*ft+c,LANES),LANES))
                        one(g,*(ib[q+3*t_].at[b] for t_ in range(3)),*(ob[q+3*t_].at[b] for t_ in range(3)),at)
            return 0
        lax.fori_loop(0,nf,tile,0)
        for c in writes(t): c.start()
        return 0
    lax.fori_loop(0,N,unit,0)
    for t in range(max(N-depth,0),N):
        for c in writes(jnp.int32(t)): c.wait()
def adam(f,gs,plan,state,before,n,ft=256,sub=2,depth=3):
    S=round((n//2)**0.5); rows,F=state[0].shape[1:]; z=Shards(n,rows*2*S,F,ft); nf=z.nf; D=z.D
    rs=S//sub; alias=len(before); k=1+len(gs)+9; el=len(plan)*3*rows*F
    buf=lambda a,q:pltpu.VMEM((depth,rs*z.rg,F) if q%3<2 else (depth,nf,rs*z.rd,D),a.dtype)
    return pl.pallas_call(functools.partial(adam_body,z=z,plan=plan,ng=len(gs),alias=alias,sub=sub,depth=depth),
        in_specs=[VM]+[ANY]*(len(gs)+9+alias),out_specs=[ANY]*9,
        scratch_shapes=[pltpu.VMEM((depth,nf,rs,*z.blk),BF)]+[buf(a,q) for q,a in enumerate(state)]*2+[DMA((depth,10)),DMA((depth,9))],
        out_shape=[jax.ShapeDtypeStruct(a.shape,a.dtype) for a in state],input_output_aliases={k+q:q for q in range(alias)},
        compiler_params=pltpu.CompilerParams(vmem_limit_bytes=67043328),name="adamw",
        cost_estimate=pl.CostEstimate(flops=20*el,bytes_accessed=22*el,transcendentals=el))(f,*gs,*state,*before)

def solution(mesh):
    n=mesh.shape["dp"]; S=round((n//2)**0.5); hf=2*S
    at=lambda x,y,c:(x%S*S+y%S)*2+c
    def turn(d):
        return [(at(x,y,c),at(x+d*(1-c),y+d*c,c)) for x in range(S) for y in range(S) for c in range(2)]
    swap=[(i,i^1) for i in range(n)]
    def step(x,dy,*arrays):
        w,m,v=(arrays[i:i+3] for i in (0,3,6))
        L,D,F=w[0].shape; count=sum(a.size for a in w); nf=F//256; nleft=nf-len(K2_POINTS[1])
        gate,up,h1,a1,a0T=k1(x[0],*w)
        G1,ss,left,dh=k2(a1,dy[0],h1,*w,n,1,K2_POINTS)
        P,f,G1=k3(a0T,dh,gate,up,w[2],ss,left,G1,n,0,count,K3_POINTS,nleft=nleft)
        state=[a.reshape(L,nf,hf,-1,D) if k%3==2 else a.reshape(L*hf,-1,F) for k,a in enumerate((*w,*m,*v))]
        move=lambda a,p:lax.ppermute(a,"dp",p)
        near=[move(P,turn(d)) for d in range(1,S)]; theirs=move(P,swap)
        out=adam(f,[G1,P],[(1,h,q,0) for h in range(2) for q in range(S)]+[(0,None,(0,0),1)],state,[],n)
        near,theirs,out=lax.optimization_barrier((near,theirs,out))
        far=[move(a,swap) for a in near]
        out=adam(f,[theirs,*near],[(0,None,(1,0),0)]+[(0,None,(0,d),d) for d in range(1,S)],state,out,n)
        far,out=lax.optimization_barrier((far,out))
        out=adam(f,far,[(0,None,(1,d),d-1) for d in range(1,S)],state,out,n)
        return tuple(o.reshape(a.shape) for o,a in zip(out,arrays))
    P=PartitionSpec
    return jax.shard_map(step,mesh=mesh,in_specs=(P(("rep","dp"),None,None),)*2+(P(None,None,None),)*9,
        out_specs=(P("rep",None,None),)*9,check_vma=False)
```

```python
import functools
import jax, jax.numpy as jnp
from jax import lax
from jax.experimental import pallas as pl
from jax.experimental.pallas import tpu as pltpu
from jax.sharding import PartitionSpec
F32,BF=jnp.float32,jnp.bfloat16
ANY=pl.BlockSpec(memory_space=pl.ANY)
VM=pl.BlockSpec(memory_space=pltpu.VMEM)
def dot(a,b,dims=((1,),(0,))):
    return lax.dot_general(a,b,(dims,((),())),preferred_element_type=F32)
NT=((1,),(1,)); TN=((0,),(0,))
def norm_scale(wide): return lax.rsqrt(jnp.mean(wide*wide,-1,keepdims=True)+1e-6)
def normed(h):
    wide=h.astype(F32); return (wide*norm_scale(wide)).astype(BF)
def sigmoid(g): return 0.5*jnp.tanh(0.5*g)+0.5

def k1_body(x_ref,wg_h,wu_h,wd_h,gate_h,up_h,h_ref,a_ref,aT_ref,wg,wu,wd,gate,up,act,wsem,osem,*,fc,L):
    i=pl.program_id(0); bm=x_ref.shape[0]; nc=wg.shape[1]//fc; last=pl.num_programs(0)-1
    cols=[pl.ds(c*fc,fc) for c in range(nc)]; copy=pltpu.make_async_copy
    loads=[[copy(h.at[L,:,s],w.at[:,s],wsem.at[q,c]) for q,(h,w) in enumerate(((wg_h,wg),(wu_h,wu)))] for c,s in enumerate(cols)]
    down=copy(wd_h.at[L],wd,wsem.at[2,0])
    stores=lambda t:[[copy(b.at[c],h.at[pl.ds(pl.multiple_of(t*bm,bm),bm),s],osem.at[q,c]) for q,(b,h) in enumerate(((gate,gate_h),(up,up_h)))] for c,s in enumerate(cols)]
    def work(first):
        x=x_ref[...]; a=normed(x)
        for c,s in enumerate(cols):
            if first:
                for w in loads[c]: w.wait()
            g=dot(a,wg[:,s]); u=dot(a,wu[:,s])
            gate[c]=g; up[c]=u
            act[:,s]=(g*sigmoid(g)*u).astype(BF)
            for w in stores(i)[c]: w.start()
        aT_ref[...]=a.T
        if first: down.wait()
        d=dot(act[...],wd[...]).astype(BF)
        h=(x.astype(F32)+d.astype(F32)).astype(BF)
        h_ref[...]=h; a_ref[...]=normed(h)
    @pl.when(i==0)
    def _():
        for c in range(nc):
            for w in loads[c]: w.start()
        down.start()
        work(True)
    @pl.when(i>0)
    def _():
        for c in stores(i-1):
            for w in c: w.wait()
        work(False)
    @pl.when(i==last)
    def _():
        for c in stores(i):
            for w in c: w.wait()
def k1(x,wg,wu,wd,L=0,bm=512,fc=768):
    T,D=x.shape; F=wg.shape[2]
    row=lambda c:pl.BlockSpec((bm,c),lambda i:(i,0))
    return pl.pallas_call(functools.partial(k1_body,fc=fc,L=L),grid=(T//bm,),
        in_specs=[row(D),ANY,ANY,ANY],out_specs=[ANY,ANY,row(D),row(D),pl.BlockSpec((D,bm),lambda i:(0,i))],
        out_shape=[jax.ShapeDtypeStruct((T,F),F32)]*2+[jax.ShapeDtypeStruct((T,D),BF)]*2+[jax.ShapeDtypeStruct((D,T),BF)],
        scratch_shapes=[pltpu.VMEM((D,F),BF),pltpu.VMEM((D,F),BF),pltpu.VMEM((F,D),BF),pltpu.VMEM((F//fc,bm,fc),F32),pltpu.VMEM((F//fc,bm,fc),F32),
            pltpu.VMEM((bm,F),BF),pltpu.SemaphoreType.DMA((3,F//fc)),pltpu.SemaphoreType.DMA((2,F//fc))],
        compiler_params=pltpu.CompilerParams(vmem_limit_bytes=60<<20),name="k1",
        cost_estimate=pl.CostEstimate(flops=6*T*D*F,bytes_accessed=10*T*F,transcendentals=T*F))(x,wg,wu,wd)


MESH=pl.DeviceIdType.MESH
DMA=pltpu.SemaphoreType.DMA
LANES=128

class Shards:
    def __init__(s,n,D,F,ft):
        s.n=n; s.side=round((n//2)**0.5); s.D,s.F,s.ft=D,F,ft; s.nf=F//ft
        s.rg=D//n; s.rd=ft//n; s.part=s.rg*ft//LANES; s.blk=(3*s.part,LANES)
        assert 2*s.side*s.side==n and s.rg*n==D and s.rd*n==ft and ft%LANES==0 and D%LANES==0

class Place:
    def __init__(s,S):
        me=lax.axis_index("dp"); c=me%2; y=(me//2)%S; x=me//(2*S)
        s.S,s.c,s.u,s.v=S,c,x*(1-c)+y*c,y*(1-c)+x*c
        s.partner=me+1-2*c; s.right=s.dev(s.u+1,s.v); s.left=s.dev(s.u+S-1,s.v)
        s.vpeer=[s.dev(s.u,s.v+d) for d in range(1,S)]; s.upeer=[s.dev(s.u+d,s.v) for d in range(1,S)]
    def place(s,layer,other,d):
        S,c=s.S,s.c; return (layer*2+(1-c if other else c))*S+((s.v if other else s.u)+S-d)%S
    def dev(s,u,v):
        S,c=s.S,s.c; u,v=u%S,v%S
        return ((u*(1-c)+v*c)*S+v*(1-c)+u*c)*2+c
    def greet(s,peers):
        b=pltpu.get_barrier_semaphore()
        for d in peers: pl.semaphore_signal(b,inc=1,device_id={"dp":d},device_id_type=MESH)

def send(src,dst,a,b,dev):
    return pltpu.make_async_remote_copy(src_ref=src,dst_ref=dst,send_sem=a,recv_sem=b,device_id={"dp":dev},device_id_type=MESH)
def wide(r): return r[...].astype(F32)

class Scatter:
    N=13
    @staticmethod
    def scratch(z,nl,ns):
        S,nf,blk=z.side,z.nf,z.blk
        V=lambda *s,dt=BF:pltpu.VMEM(s+blk,dt)
        return [V(nl,2,S,S),V(nf,S,S),V(nf,S-1,S),V(nf,S-1),V(ns,S-1,S),V(ns,S-1),V(ns,dt=F32),DMA((nf,)),DMA((nf,)),*[DMA((nf,S-1))]*4]
    def __init__(s,z,pos,nl,ns,refs):
        s.z,s.pos,s.nl,s.ns=z,pos,nl,ns
        (s.loc,s.rc,s.fu,s.fv,s.su,s.sv,s.own,s.cS,s.cR,s.uS,s.uR,s.vS,s.vR)=refs
    def copies(s,i,k):
        o=s.pos; n=lax.rem(k,s.nl); p=lax.rem(k,s.ns)
        if i==0: return [send(s.loc.at[n,1-o.c],s.rc.at[k],s.cS.at[k],s.cR.at[k],o.partner)]
        if i==1: return [send(s.su.at[p,d],s.fu.at[k,d],s.uS.at[k,d],s.uR.at[k,d],to) for d,to in enumerate(o.upeer)]
        if i==2: return [send(s.sv.at[p,d],s.fv.at[k,d],s.vS.at[k,d],s.vR.at[k,d],to) for d,to in enumerate(o.vpeer)]
    def step(s,i,k,done=None):
        o=s.pos; S=o.S; n=lax.rem(k,s.nl); p=lax.rem(k,s.ns); u,v,c=o.u,o.v,o.c
        if i>0:
            for d in s.copies(i-1,k): d.wait()
        both=lambda q,sl:wide(s.loc.at[n,c,q,sl])+wide(s.rc.at[k,q,sl])
        if i==1:
            for d in range(S-1): s.su[p,d]=both((u+d+1)%S,pl.ds(0,S)).astype(BF)
        if i==2:
            def one(r):
                t=both(u,r)
                for d in range(S-1): t=t+wide(s.fu.at[k,d,r])
                return t
            for d in range(S-1): s.sv[p,d]=one((v+d+1)%S).astype(BF)
            s.own[p]=one(v)
        if i==3:
            g=s.own[p]
            for d in range(S-1): g=g+wide(s.fv.at[k,d])
            done(k,g.astype(BF))
        if i<3:
            for d in s.copies(i,k): d.start()
    def store(s,k,a,part):
        z=s.z; S=z.side; n=lax.rem(k,s.nl); r=z.rd if part==2 else z.rg
        for i in range(z.n):
            rows=a[i*r:(i+1)*r]
            s.loc[n,i//(S*S),i//S%S,i%S,pl.ds(part*z.part,z.part)]=jnp.concatenate([rows[:,b:b+LANES] for b in range(0,a.shape[1],LANES)],0).astype(BF)

class Gather:
    N=10
    @staticmethod
    def scratch(z,count):
        S=z.side
        return [pltpu.VMEM((count,S,*z.blk),BF),*[DMA((count,S-1))]*2,*[DMA((count,2))]*4,*[DMA((count,))]*3]
    def __init__(s,z,pos,first,Q,refs):
        s.z,s.pos,s.first,s.Q=z,pos,first,Q
        (s.P,s.wS,s.wR,s.aS,s.aR,s.bS,s.bR,s.cS,s.cR,s.lS)=refs
    def copies(s,i,k,here=False):
        o=s.pos; S=o.S; h=S//2; u,v,c=o.u,o.v,o.c; q=k+s.first; l,r=(u+S-1)%S,(u+1)%S; P,Q=s.P,s.Q
        A,B=pl.ds(0,h),pl.ds(h,h)
        if i==0: return [send(P.at[k,v],P.at[k,(v+S-d)%S if here else v],s.wS.at[k,d-1],s.wR.at[k,d-1],o.vpeer[d-1]) for d in range(1,S)]
        if i==1: return [send(P.at[k],Q.at[c,q,(l,r)[w] if here else u],s.aS.at[k,w],s.aR.at[k,w],d) for w,d in enumerate((o.right,o.left))]
        if i==2: return [send(Q.at[c,q,(l,r)[w],(A,B)[w]],Q.at[c,q,(u+h)%S if here else (l,r)[w],(A,B)[w]],s.bS.at[k,w],s.bR.at[k,w],d) for w,d in enumerate((o.right,o.left))]
        if i==3: return [send(Q.at[c,q],Q.at[1-c if here else c,q],s.cS.at[k],s.cR.at[k],o.partner)]
    def keep(s,k): return pltpu.make_async_copy(s.P.at[k],s.Q.at[s.pos.c,k+s.first,s.pos.u],s.lS.at[k])
    def step(s,i,k):
        if i>0:
            for d in s.copies(i-1,k,True): d.wait()
        if i==1: s.keep(k).start()
        if i==3: s.keep(k).wait()
        if i<4:
            for d in s.copies(i,k): d.start()

def run(points,p,parity,do):
    if not any(t%2==parity for t in points): return
    upto=lambda q:sum((q>=t).astype(jnp.int32) for t in points)
    lax.fori_loop(upto(p-1),upto(p),lambda k,_:(do(k),0)[1],0)

def elementwise(g,u,da):
    sg=sigmoid(g); silu=g*sg
    return (silu*u).astype(BF),(da*u*(sg+silu*(1.0-sg))).astype(BF),(da*silu).astype(BF)

def check_points(rs,nl,ns,later):
    nf=len(rs)
    for k in range(nf):
        assert rs[k][0]==2*(k+later)+1 and all(a<b for a,b in zip(rs[k],rs[k][1:])),rs[k]
        if k>=nl: assert rs[k-nl][2]<2*(k+later)
        if k>=ns: assert all(rs[k-ns][i+1]<=rs[k][i] for i in (1,2))
        if k: assert all(a<=b for a,b in zip(rs[k-1],rs[k]))
def check_gather(ag,starts=None):
    for k,t in enumerate(ag):
        assert all(a<b for a,b in zip(t,t[1:])) and (not starts or t[0]==starts[k]),t
        if k: assert all(a<=b for a,b in zip(ag[k-1],t))

def k2_body(a_ref,dy_ref,h_ref,wg_h,wu_h,wd_h,Q,ss_ref,left_ref,dh_ref,wg,wu,wd,aT,dg,du,act,sem,*refs,z,nl,ns,rc,bc,L,rs,ag):
    j=pl.program_id(0); T,D=a_ref.shape; nf,ft=z.nf,z.ft; na=len(ag); nb=T//bc
    o=Place(z.side); sc=Scatter(z,o,nl,ns,refs[:Scatter.N]); ga=Gather(z,o,0,Q,refs[Scatter.N:])
    def done(k,g):
        w=g.astype(F32); ss_ref[...]+=w*w
        @pl.when(k<na)
        def _(): ga.P[k,o.v]=g; ga.step(0,k)
        if na<nf:
            @pl.when(k>=na)
            def _(): left_ref[k-na]=g
    def point(p,parity):
        for i in (3,2,1,0): run([t[i] for t in rs],p,parity,lambda k:sc.step(i,k,done))
        for i in (4,3,2,1): run([t[i] for t in ag],p,parity,lambda k:ga.step(i,k))
    def cps(t):
        s=pl.ds(pl.multiple_of(t*ft,ft),ft)
        return [pltpu.make_async_copy(wg_h.at[L,:,s],wg.at[:,s],sem.at[0,t]),pltpu.make_async_copy(wu_h.at[L,:,s],wu.at[:,s],sem.at[1,t]),
                pltpu.make_async_copy(wd_h.at[L,s,:],wd.at[lax.rem(t,2)],sem.at[2,t])]
    @pl.when(j==0)
    def _():
        o.greet((o.partner,*o.upeer,*o.vpeer))
        for c in cps(0): c.start()
        for t in range(1,nf):
            for c in cps(t)[:2]: c.start()
        ss_ref[...]=jnp.zeros_like(ss_ref)
        for r in range(0,T,rc): aT[:,pl.ds(r,rc)]=a_ref[pl.ds(r,rc),:].T
    s=pl.ds(pl.multiple_of(lax.rem(j,nf)*ft,ft),ft)
    @pl.when(j<nf)
    def _():
        for c in cps(j): c.wait()
        @pl.when(j+1<nf)
        def _(): cps(j+1)[2].start()
        wgt,wut,wdt=wg[:,s],wu[:,s],wd[lax.rem(j,2)]
        for r in range(0,T,rc):
            rs_=pl.ds(r,rc); a=a_ref[rs_,:]
            g=dot(a,wgt); u=dot(a,wut); da=dot(dy_ref[rs_,:],wdt,NT).astype(BF).astype(F32)
            act[rs_,:],dg[rs_,s],du[rs_,s]=elementwise(g,u,da)
    @pl.when(j==0)
    def _(): pl.semaphore_wait(pltpu.get_barrier_semaphore(),1+len(o.upeer)+len(o.vpeer))
    point(2*j,0)
    @pl.when(j<nf)
    def _():
        sc.store(j,dot(aT[...],dg[:,s]),0)
        sc.store(j,dot(aT[...],du[:,s]),1)
        sc.store(j,dot(act[...],dy_ref[...],TN),2)
    @pl.when((j>=nf)&(j<nf+nb))
    def _():
        rs_=pl.ds(pl.multiple_of((j-nf)*bc,bc),bc)
        da=(dot(dg[rs_,:],wg[...],NT).astype(BF).astype(F32)+dot(du[rs_,:],wu[...],NT).astype(BF).astype(F32)).astype(BF).astype(F32)
        x=h_ref[...].astype(F32); scale=norm_scale(x)
        t=jnp.sum(da*x,-1,keepdims=True)*(1.0/D)
        dn=(da*scale-x*(scale*scale*scale*t)).astype(BF).astype(F32)
        dh_ref[...]=(dy_ref[rs_,:].astype(F32)+dn).astype(BF)
    point(2*j+1,1)
def k2(a1,dy,h1,wg,wu,wd,n,L,points,ft=256,rc=512,bc=256,nl=4,ns=3):
    T,D=a1.shape; F=wg.shape[2]; z=Shards(n,D,F,ft); nf=z.nf; nb=T//bc; S=z.side
    rs,ag=points; steps=max(nf+nb,max(t[-1] for t in rs+ag)//2+1); check_points(rs,nl,ns,0); check_gather(ag,[t[3] for t in rs]); nleft=max(nf-len(ag),1)
    back=pl.BlockSpec((bc,D),lambda j:(jnp.clip(j-nf,0,nb-1),0)); all_=lambda *s:pl.BlockSpec(s,lambda j:(0,)*len(s))
    return pl.pallas_call(functools.partial(k2_body,z=z,nl=nl,ns=ns,rc=rc,bc=bc,L=L,rs=rs,ag=ag),grid=(steps,),
        in_specs=[VM,VM,back,ANY,ANY,ANY],out_specs=[ANY,all_(*z.blk),all_(nleft,*z.blk),back],
        out_shape=[jax.ShapeDtypeStruct((2,nf,S,S,*z.blk),BF),jax.ShapeDtypeStruct(z.blk,F32),jax.ShapeDtypeStruct((nleft,*z.blk),BF),jax.ShapeDtypeStruct((T,D),BF)],
        scratch_shapes=[pltpu.VMEM((D,F),BF),pltpu.VMEM((D,F),BF),pltpu.VMEM((2,ft,D),BF),pltpu.VMEM((D,T),BF),
                        pltpu.VMEM((T,F),BF),pltpu.VMEM((T,F),BF),pltpu.VMEM((T,ft),BF),DMA((3,nf)),*Scatter.scratch(z,nl,ns),*Gather.scratch(z,max(len(ag),1))],
        compiler_params=pltpu.CompilerParams(vmem_limit_bytes=67043328,collective_id=1,has_side_effects=True),name="k2",
        cost_estimate=pl.CostEstimate(flops=16*T*D*F,bytes_accessed=30<<20,transcendentals=T*F))(a1,dy,h1,wg,wu,wd)

def k3_body(aT_h,dh_ref,g_ref,u_ref,wd_ref,ss_ref,left_ref,Q1_,P_out,f_ref,Q1,P_ref,aT,dg,du,act,sq,nsend,nplane,nc,nS,nR,gS,gR,oS,sem,*refs,z,nl,ns,rc,count,rs,ag,left,sqp):
    j=pl.program_id(0); D,T=aT.shape; nf,S=z.nf,z.side
    o=Place(S); sc=Scatter(z,o,nl,ns,refs[:Scatter.N])
    nleft=len(left); gl=Gather(z,o,nf-nleft,Q1,refs[Scatter.N:]) if nleft else None
    apart=[(a,b) for a in range(S) for b in range(S) if a or b]; plane=[o.dev(o.u+a,o.v+b) for a,b in apart]
    to=lambda k,here=False:[send(P_ref.at[k,o.v],P_ref.at[k,(o.v+S-d)%S if here else o.v],gS.at[k,d-1],gR.at[k,d-1],o.vpeer[d-1]) for d in range(1,S)]
    def done(k,g):
        w=g.astype(F32); sq[...]+=w*w
        P_ref[k,o.v]=g
        for d in to(k): d.start()
    def there(k):
        for d in to(k,True): d.wait()
        give(k).start()
    give=lambda k:pltpu.make_async_copy(P_ref.at[k],P_out.at[k],oS.at[k])
    def reduce_(p,parity):
        for i in (3,2,1,0): run([t[i] for t in rs],p,parity,lambda k:sc.step(i,k,done))
    def rest(p,parity):
        if nleft:
            for i in (4,3,2,1,0): run([t[i] for t in left],p,parity,lambda k:gl.step(i,k))
        run([t[1] for t in ag],p,parity,there)
    load=pltpu.make_async_copy(aT_h,aT,sem)
    def front(rows,b):
        for r in rows:
            rs_=pl.ds(r,rc)
            da=dot(dh_ref[rs_,:],wd_ref[...],NT).astype(BF).astype(F32)
            act[b,rs_,:],dg[b,rs_,:],du[b,rs_,:]=elementwise(g_ref[rs_,:],u_ref[rs_,:],da)
    def back(k,part,b):
        if part<2: sc.store(k,dot(aT[...],(dg,du)[part][b]),part)
        else: sc.store(k,dot(act[b],dh_ref[...],TN),2)
    rows=range(0,T,rc); half=len(rows)//2; b=lax.rem(j,2)
    @pl.when(j==0)
    def _():
        load.start()
        o.greet((o.partner,*plane))
        sq[...]=ss_ref[...]
        for k in range(nleft): gl.P[k,o.v]=left_ref[k]
        front(rows[:half],b)
    @pl.when((j>0)&(j<nf))
    def _():
        front(rows[:half],b); back(j-1,0,1-b)
    @pl.when(j==nf)
    def _(): back(j-1,0,1-b)
    @pl.when(j==0)
    def _(): pl.semaphore_wait(pltpu.get_barrier_semaphore(),1+len(plane))
    reduce_(2*j,0); rest(2*j,0)
    @pl.when(j==0)
    def _():
        front(rows[half:],b); load.wait()
    @pl.when((j>0)&(j<nf))
    def _():
        back(j-1,1,1-b); front(rows[half:],b); back(j-1,2,1-b)
    @pl.when(j==nf)
    def _(): back(j-1,1,1-b); back(j-1,2,1-b)
    p=2*j+1
    reduce_(p,1)
    def sums(buf,at,peers,b): return [send(nsend.at[b],buf.at[a],nS.at[b,i],nR.at[b,i],d) for i,(a,d) in enumerate(zip(at,peers))]
    hops=((nplane,o.u*S+o.v,plane,[(o.u+S-a)%S*S+(o.v+S-b)%S for a,b in apart],S*S),(nc,o.c,[o.partner],[1-o.c],2))
    for b_ in range(3):
        @pl.when(p==sqp[b_])
        def _(b=b_):
            if b==0: t=jnp.broadcast_to(jnp.sum(jnp.sum(sq[...],0,keepdims=True),1,keepdims=True),(8,128))
            else:
                buf,_,peers,at,k=hops[b-1]
                for d in sums(buf,at,peers,b-1): d.wait()
                t=buf[0]
                for i in range(1,k): t=t+buf[i]
            if b<2:
                buf,mine,peers,_,_=hops[b]
                nsend[b]=t; buf[mine]=t
                for d in sums(buf,[mine]*len(peers),peers,b): d.start()
            else: f_ref[...]=jnp.minimum(1.0,0.5*lax.rsqrt(t*(1.0/count)+1e-30))
    rest(p,1)
    @pl.when(j==pl.num_programs(0)-1)
    def _():
        for k in range(nf): give(k).wait()
def k3(a0T,dh,gate,up,wd,ss,left,Q1,n,L,count,points,ft=256,rc=512,nl=6,ns=4,nleft=2):
    D,T=a0T.shape; F=gate.shape[1]; z=Shards(n,D,F,ft); nf=z.nf; S=z.side
    rs,ag,lp,sqp=points; steps=max(max(t[-1] for t in rs+ag+lp),sqp[-1])//2+1
    assert len(lp)==nleft
    check_points(rs,nl,ns,1); check_gather(ag,[t[3] for t in rs]); check_gather(lp)
    cl=lambda j:jnp.minimum(j,nf-1); all_=lambda *s:pl.BlockSpec(s,lambda j:(0,)*len(s))
    col=lambda r:pl.BlockSpec((r,ft),lambda j:(0,cl(j)))
    return pl.pallas_call(functools.partial(k3_body,z=z,nl=nl,ns=ns,rc=rc,count=count,rs=rs,ag=ag,left=lp,sqp=sqp),grid=(steps,),
        in_specs=[ANY,VM,col(T),col(T),pl.BlockSpec((None,ft,D),lambda j:(L,cl(j),0)),VM,VM,ANY],
        out_specs=[ANY,all_(8,128),ANY],
        out_shape=[jax.ShapeDtypeStruct((nf,S,*z.blk),BF),jax.ShapeDtypeStruct((8,128),F32),jax.ShapeDtypeStruct(Q1.shape,BF)],input_output_aliases={7:2},
        scratch_shapes=[pltpu.VMEM((nf,S,*z.blk),BF),pltpu.VMEM((D,T),BF)]+[pltpu.VMEM((2,T,ft),BF)]*3+[pltpu.VMEM(z.blk,F32),pltpu.VMEM((2,8,128),F32),pltpu.VMEM((S*S,8,128),F32),
            pltpu.VMEM((2,8,128),F32),DMA((2,S*S)),DMA((2,S*S)),DMA((nf,S-1)),DMA((nf,S-1)),DMA((nf,)),DMA,*Scatter.scratch(z,nl,ns),*(Gather.scratch(z,nleft) if nleft else [])],
        compiler_params=pltpu.CompilerParams(vmem_limit_bytes=67043328,collective_id=2,has_side_effects=True),name="k3",
        cost_estimate=pl.CostEstimate(flops=8*T*D*F,bytes_accessed=10*T*F,transcendentals=T*F))(a0T,dh,gate,up,wd,ss,left,Q1)


def points(rows):
    return [[ord(c) - ord("0") for c in row] for row in rows.split(",")]


K2_POINTS = (points("1257,3479,569;,78;=,9:=?,;<?A,=>AG,?@GM,ACKQ"), points("79=?A,9;?CG,;=AGK,=?EMQ,?AIOS"))
K3_POINTS = (points("359<,57;>,79=A,9;?B,;<AI,=?EQ,?AKW,ACOY,CGS]"), points("<?,>A,AG,BM,IU,Q[,W_,Ya,]c"), points("036:;,047;=,047<=,048<>"), points("]eg")[0])

def adam_body(f_ref,*refs,z,plan,ng,alias,sub,depth):
    gs,refs=refs[:ng],refs[ng:]; ins=refs[:9]; outs=refs[9+alias:18+alias]
    gb,refs=refs[18+alias],refs[19+alias:]; ib,ob,(isem,osem)=refs[:9],refs[9:18],refs[18:]
    S,ft,rg,rd,nf=z.side,z.ft,z.rg,z.rd,z.nf; rs=S//sub; hf=2*S; N=len(plan)*sub
    f=f_ref[0:1,0:1]; o=Place(S)
    places=[(l*2+h)*S+part if h is not None else o.place(l,*part) for l,h,part,_ in plan]
    def at(ref,q,t):
        p=sum(jnp.where(t//sub==k,place,0) for k,place in enumerate(places)); h=lax.rem(t,sub)
        if q%3<2: return ref.at[p,pl.ds(pl.multiple_of(h*(rs*rg),8),rs*rg)]
        return ref.at[p//hf,:,lax.rem(p,hf),pl.ds(pl.multiple_of(h*(rs*rd),8),rs*rd)]
    def reads(t):
        b=lax.rem(t,depth); return [pltpu.make_async_copy(at(ins[q],q,t),ib[q].at[b],isem.at[b,q]) for q in range(9)]
    def writes(t):
        b=lax.rem(t,depth); return [pltpu.make_async_copy(ob[q].at[b],at(outs[q],q,t),osem.at[b,q]) for q in range(9)]
    def gread(ref,part,t):
        b=lax.rem(t,depth); h=lax.rem(t,sub)
        src=(ref if part is None else ref.at[part[0],:,part[1]]).at[:,pl.ds(h*rs,rs)]
        return pltpu.make_async_copy(src,gb.at[b],isem.at[b,9])
    def fetch(t):
        for c in reads(t): c.start()
        for k,(_,h,part,a) in enumerate(plan):
            @pl.when(t//sub==k)
            def _(a=a,part=None if h is None else (h,part)): gread(gs[a],part,t).start()
    def one(g,w,m,v,wo,mo,vo,at):
        g=g.astype(F32)*f
        m=0.9*m[at]+0.1*g
        v=0.95*v[at]+0.05*g*g
        w=w[at].astype(F32)
        wo[at]=(w-0.02*(m*lax.rsqrt(v+1e-8)+0.1*w)).astype(BF); mo[at]=m; vo[at]=v
    for t in range(depth-1): fetch(jnp.int32(t))
    def unit(t,_):
        b=lax.rem(t,depth)
        @pl.when(t+depth-1<N)
        def _(): fetch(t+depth-1)
        for c in reads(t): c.wait()
        pltpu.make_async_copy(gb.at[b],gb.at[b],isem.at[b,9]).wait()
        @pl.when(t>=depth)
        def _():
            for c in writes(t-depth): c.wait()
        def tile(k,_):
            for r in range(rs):
                for q in range(3):
                    rows,cols=(rd,z.D) if q==2 else (rg,ft)
                    for c in range(0,cols,LANES):
                        g=gb[b,k,r,pl.ds(q*z.part+c//LANES*rows,rows),:]
                        at=(k,pl.ds(r*rows,rows),pl.ds(c,LANES)) if q==2 else (pl.ds(r*rows,rows),pl.ds(pl.multiple_of(k*ft+c,LANES),LANES))
                        one(g,*(ib[q+3*t_].at[b] for t_ in range(3)),*(ob[q+3*t_].at[b] for t_ in range(3)),at)
            return 0
        lax.fori_loop(0,nf,tile,0)
        for c in writes(t): c.start()
        return 0
    lax.fori_loop(0,N,unit,0)
    for t in range(max(N-depth,0),N):
        for c in writes(jnp.int32(t)): c.wait()
def adam(f,gs,plan,state,before,n,ft=256,sub=2,depth=4):
    S=round((n//2)**0.5); rows,F=state[0].shape[1:]; z=Shards(n,rows*2*S,F,ft); nf=z.nf; D=z.D
    rs=S//sub; alias=len(before); k=1+len(gs)+9; el=len(plan)*3*rows*F
    buf=lambda a,q:pltpu.VMEM((depth,rs*z.rg,F) if q%3<2 else (depth,nf,rs*z.rd,D),a.dtype)
    return pl.pallas_call(functools.partial(adam_body,z=z,plan=plan,ng=len(gs),alias=alias,sub=sub,depth=depth),
        in_specs=[VM]+[ANY]*(len(gs)+9+alias),out_specs=[ANY]*9,
        scratch_shapes=[pltpu.VMEM((depth,nf,rs,*z.blk),BF)]+[buf(a,q) for q,a in enumerate(state)]*2+[DMA((depth,10)),DMA((depth,9))],
        out_shape=[jax.ShapeDtypeStruct(a.shape,a.dtype) for a in state],input_output_aliases={k+q:q for q in range(alias)},
        compiler_params=pltpu.CompilerParams(vmem_limit_bytes=67043328),name="adamw",
        cost_estimate=pl.CostEstimate(flops=20*el,bytes_accessed=22*el,transcendentals=el))(f,*gs,*state,*before)

def solution(mesh):
    n=mesh.shape["dp"]; S=round((n//2)**0.5); hf=2*S
    at=lambda x,y,c:(x%S*S+y%S)*2+c
    def turn(d):
        return [(at(x,y,c),at(x+d*(1-c),y+d*c,c)) for x in range(S) for y in range(S) for c in range(2)]
    swap=[(i,i^1) for i in range(n)]
    def step(x,dy,*arrays):
        w,m,v=(arrays[i:i+3] for i in (0,3,6))
        L,D,F=w[0].shape; count=sum(a.size for a in w); nf=F//256; nleft=nf-len(K2_POINTS[1])
        gate,up,h1,a1,a0T=k1(x[0],*w)
        G1,ss,left,dh=k2(a1,dy[0],h1,*w,n,1,K2_POINTS)
        P,f,G1=k3(a0T,dh,gate,up,w[2],ss,left,G1,n,0,count,K3_POINTS,nleft=nleft)
        state=[a.reshape(L,nf,hf,-1,D) if k%3==2 else a.reshape(L*hf,-1,F) for k,a in enumerate((*w,*m,*v))]
        move=lambda a,p:lax.ppermute(a,"dp",p)
        near=[move(P,turn(d)) for d in range(1,S)]; theirs=move(P,swap)
        out=adam(f,[G1,P],[(1,h,q,0) for h in range(2) for q in range(S)]+[(0,None,(0,0),1)],state,[],n)
        near,theirs,out=lax.optimization_barrier((near,theirs,out))
        far=[move(a,swap) for a in near]
        out=adam(f,[theirs,*near],[(0,None,(1,0),0)]+[(0,None,(0,d),d) for d in range(1,S)],state,out,n)
        far,out=lax.optimization_barrier((far,out))
        out=adam(f,far,[(0,None,(1,d),d-1) for d in range(1,S)],state,out,n)
        return tuple(o.reshape(a.shape) for o,a in zip(out,arrays))
    P=PartitionSpec
    return jax.shard_map(step,mesh=mesh,in_specs=(P(("rep","dp"),None,None),)*2+(P(None,None,None),)*9,
        out_specs=(P("rep",None,None),)*9,check_vma=False)
```

```python
import functools
import jax, jax.numpy as jnp
from jax import lax
from jax.experimental import pallas as pl
from jax.experimental.pallas import tpu as pltpu
from jax.sharding import PartitionSpec
F32,BF=jnp.float32,jnp.bfloat16
ANY=pl.BlockSpec(memory_space=pl.ANY)
VM=pl.BlockSpec(memory_space=pltpu.VMEM)
def dot(a,b,dims=((1,),(0,))):
    return lax.dot_general(a,b,(dims,((),())),preferred_element_type=F32)
NT=((1,),(1,)); TN=((0,),(0,))
def norm_scale(wide): return lax.rsqrt(jnp.mean(wide*wide,-1,keepdims=True)+1e-6)
def normed(h):
    wide=h.astype(F32); return (wide*norm_scale(wide)).astype(BF)
def sigmoid(g): return 0.5*jnp.tanh(0.5*g)+0.5

def k1_body(x_ref,wg,wu,wd,gate_ref,up_ref,h_ref,a_ref,aT_ref,act,*,fc):
    x=x_ref[...]; a=normed(x); F=wg.shape[1]; aT_ref[...]=a.T
    for c in range(F//fc):
        s=pl.ds(c*fc,fc)
        g=dot(a,wg[:,s]); u=dot(a,wu[:,s])
        gate_ref[:,s]=g; up_ref[:,s]=u
        act[:,s]=(g*sigmoid(g)*u).astype(BF)
    d=dot(act[...],wd[...]).astype(BF)
    h=(x.astype(F32)+d.astype(F32)).astype(BF)
    h_ref[...]=h; a_ref[...]=normed(h)
def k1(x,wg,wu,wd,bm=512,fc=768):
    T,D=x.shape; F=wg.shape[2]
    wspec=lambda r,c:pl.BlockSpec((None,r,c),lambda i:(0,0,0),pipeline_mode=pl.Buffered(1))
    row=lambda c:pl.BlockSpec((bm,c),lambda i:(i,0))
    return pl.pallas_call(functools.partial(k1_body,fc=fc),grid=(T//bm,),
        in_specs=[row(D),wspec(D,F),wspec(D,F),wspec(F,D)],
        out_specs=[row(F),row(F),row(D),row(D),pl.BlockSpec((D,bm),lambda i:(0,i))],
        out_shape=[jax.ShapeDtypeStruct((T,F),F32)]*2+[jax.ShapeDtypeStruct((T,D),BF)]*2+[jax.ShapeDtypeStruct((D,T),BF)],
        scratch_shapes=[pltpu.VMEM((bm,F),BF)],
        compiler_params=pltpu.CompilerParams(vmem_limit_bytes=60<<20),name="k1",
        cost_estimate=pl.CostEstimate(flops=6*T*D*F,bytes_accessed=10*T*F,transcendentals=T*F))(x,wg,wu,wd)


MESH=pl.DeviceIdType.MESH
DMA=pltpu.SemaphoreType.DMA
LANES=128

class Shards:
    def __init__(s,n,D,F,ft):
        s.n=n; s.side=round((n//2)**0.5); s.D,s.F,s.ft=D,F,ft; s.nf=F//ft
        s.rg=D//n; s.rd=ft//n; s.part=s.rg*ft//LANES; s.blk=(3*s.part,LANES)
        assert 2*s.side*s.side==n and s.rg*n==D and s.rd*n==ft and ft%LANES==0 and D%LANES==0

class Place:
    def __init__(s,S):
        me=lax.axis_index("dp"); c=me%2; y=(me//2)%S; x=me//(2*S)
        s.S,s.c,s.u,s.v=S,c,x*(1-c)+y*c,y*(1-c)+x*c
        s.partner=me+1-2*c; s.right=s.dev(s.u+1,s.v); s.left=s.dev(s.u+S-1,s.v)
        s.vpeer=[s.dev(s.u,s.v+d) for d in range(1,S)]; s.upeer=[s.dev(s.u+d,s.v) for d in range(1,S)]
    def place(s,layer,other,d):
        S,c=s.S,s.c; return (layer*2+(1-c if other else c))*S+((s.v if other else s.u)+S-d)%S
    def dev(s,u,v):
        S,c=s.S,s.c; u,v=u%S,v%S
        return ((u*(1-c)+v*c)*S+v*(1-c)+u*c)*2+c
    def greet(s,peers):
        b=pltpu.get_barrier_semaphore()
        for d in peers: pl.semaphore_signal(b,inc=1,device_id={"dp":d},device_id_type=MESH)

def send(src,dst,a,b,dev):
    return pltpu.make_async_remote_copy(src_ref=src,dst_ref=dst,send_sem=a,recv_sem=b,device_id={"dp":dev},device_id_type=MESH)
def wide(r): return r[...].astype(F32)

class Scatter:
    N=13
    @staticmethod
    def scratch(z,nl,ns):
        S,nf,blk=z.side,z.nf,z.blk
        V=lambda *s,dt=BF:pltpu.VMEM(s+blk,dt)
        return [V(nl,2,S,S),V(nf,S,S),V(nf,S-1,S),V(nf,S-1),V(ns,S-1,S),V(ns,S-1),V(ns,dt=F32),DMA((nf,)),DMA((nf,)),*[DMA((nf,S-1))]*4]
    def __init__(s,z,pos,nl,ns,refs):
        s.z,s.pos,s.nl,s.ns=z,pos,nl,ns
        (s.loc,s.rc,s.fu,s.fv,s.su,s.sv,s.own,s.cS,s.cR,s.uS,s.uR,s.vS,s.vR)=refs
    def copies(s,i,k):
        o=s.pos; n=lax.rem(k,s.nl); p=lax.rem(k,s.ns)
        if i==0: return [send(s.loc.at[n,1-o.c],s.rc.at[k],s.cS.at[k],s.cR.at[k],o.partner)]
        if i==1: return [send(s.su.at[p,d],s.fu.at[k,d],s.uS.at[k,d],s.uR.at[k,d],to) for d,to in enumerate(o.upeer)]
        if i==2: return [send(s.sv.at[p,d],s.fv.at[k,d],s.vS.at[k,d],s.vR.at[k,d],to) for d,to in enumerate(o.vpeer)]
    def step(s,i,k,done=None):
        o=s.pos; S=o.S; n=lax.rem(k,s.nl); p=lax.rem(k,s.ns); u,v,c=o.u,o.v,o.c
        if i>0:
            for d in s.copies(i-1,k): d.wait()
        both=lambda q,sl:wide(s.loc.at[n,c,q,sl])+wide(s.rc.at[k,q,sl])
        if i==1:
            for d in range(S-1): s.su[p,d]=both((u+d+1)%S,pl.ds(0,S)).astype(BF)
        if i==2:
            def one(r):
                t=both(u,r)
                for d in range(S-1): t=t+wide(s.fu.at[k,d,r])
                return t
            for d in range(S-1): s.sv[p,d]=one((v+d+1)%S).astype(BF)
            s.own[p]=one(v)
        if i==3:
            g=s.own[p]
            for d in range(S-1): g=g+wide(s.fv.at[k,d])
            done(k,g.astype(BF))
        if i<3:
            for d in s.copies(i,k): d.start()
    def store(s,k,a,part):
        z=s.z; S=z.side; n=lax.rem(k,s.nl); r=z.rd if part==2 else z.rg
        for i in range(z.n):
            rows=a[i*r:(i+1)*r]
            s.loc[n,i//(S*S),i//S%S,i%S,pl.ds(part*z.part,z.part)]=jnp.concatenate([rows[:,b:b+LANES] for b in range(0,a.shape[1],LANES)],0).astype(BF)

class Gather:
    N=10
    @staticmethod
    def scratch(z,count):
        S=z.side
        return [pltpu.VMEM((count,S,*z.blk),BF),*[DMA((count,S-1))]*2,*[DMA((count,2))]*4,*[DMA((count,))]*3]
    def __init__(s,z,pos,first,Q,refs):
        s.z,s.pos,s.first,s.Q=z,pos,first,Q
        (s.P,s.wS,s.wR,s.aS,s.aR,s.bS,s.bR,s.cS,s.cR,s.lS)=refs
    def copies(s,i,k,here=False):
        o=s.pos; S=o.S; h=S//2; u,v,c=o.u,o.v,o.c; q=k+s.first; l,r=(u+S-1)%S,(u+1)%S; P,Q=s.P,s.Q
        A,B=pl.ds(0,h),pl.ds(h,h)
        if i==0: return [send(P.at[k,v],P.at[k,(v+S-d)%S if here else v],s.wS.at[k,d-1],s.wR.at[k,d-1],o.vpeer[d-1]) for d in range(1,S)]
        if i==1: return [send(P.at[k],Q.at[c,q,(l,r)[w] if here else u],s.aS.at[k,w],s.aR.at[k,w],d) for w,d in enumerate((o.right,o.left))]
        if i==2: return [send(Q.at[c,q,(l,r)[w],(A,B)[w]],Q.at[c,q,(u+h)%S if here else (l,r)[w],(A,B)[w]],s.bS.at[k,w],s.bR.at[k,w],d) for w,d in enumerate((o.right,o.left))]
        if i==3: return [send(Q.at[c,q],Q.at[1-c if here else c,q],s.cS.at[k],s.cR.at[k],o.partner)]
    def keep(s,k): return pltpu.make_async_copy(s.P.at[k],s.Q.at[s.pos.c,k+s.first,s.pos.u],s.lS.at[k])
    def step(s,i,k):
        if i>0:
            for d in s.copies(i-1,k,True): d.wait()
        if i==1: s.keep(k).start()
        if i==3: s.keep(k).wait()
        if i<4:
            for d in s.copies(i,k): d.start()

def run(points,p,parity,do):
    if not any(t%2==parity for t in points): return
    upto=lambda q:sum((q>=t).astype(jnp.int32) for t in points)
    lax.fori_loop(upto(p-1),upto(p),lambda k,_:(do(k),0)[1],0)

def elementwise(g,u,da):
    sg=sigmoid(g); silu=g*sg
    return (silu*u).astype(BF),(da*u*(sg+silu*(1.0-sg))).astype(BF),(da*silu).astype(BF)

def check_points(rs,nl,ns,later):
    nf=len(rs)
    for k in range(nf):
        assert rs[k][0]==2*(k+later)+1 and all(a<b for a,b in zip(rs[k],rs[k][1:])),rs[k]
        if k>=nl: assert rs[k-nl][2]<2*(k+later)
        if k>=ns: assert all(rs[k-ns][i+1]<=rs[k][i] for i in (1,2))
        if k: assert all(a<=b for a,b in zip(rs[k-1],rs[k]))
def check_gather(ag,starts=None):
    for k,t in enumerate(ag):
        assert all(a<b for a,b in zip(t,t[1:])) and (not starts or t[0]==starts[k]),t
        if k: assert all(a<=b for a,b in zip(ag[k-1],t))

def k2_body(a_ref,dy_ref,h_ref,wg_h,wu_h,wd_h,Q,ss_ref,left_ref,dh_ref,wg,wu,wd,aT,dg,du,act,sem,*refs,z,nl,ns,rc,bc,L,rs,ag):
    j=pl.program_id(0); T,D=a_ref.shape; nf,ft=z.nf,z.ft; na=len(ag); nb=T//bc
    o=Place(z.side); sc=Scatter(z,o,nl,ns,refs[:Scatter.N]); ga=Gather(z,o,0,Q,refs[Scatter.N:])
    def done(k,g):
        w=g.astype(F32); ss_ref[...]+=w*w
        @pl.when(k<na)
        def _(): ga.P[k,o.v]=g; ga.step(0,k)
        if na<nf:
            @pl.when(k>=na)
            def _(): left_ref[k-na]=g
    def point(p,parity):
        for i in (3,2,1,0): run([t[i] for t in rs],p,parity,lambda k:sc.step(i,k,done))
        for i in (4,3,2,1): run([t[i] for t in ag],p,parity,lambda k:ga.step(i,k))
    def cps(t):
        s=pl.ds(pl.multiple_of(t*ft,ft),ft)
        return [pltpu.make_async_copy(wg_h.at[L,:,s],wg.at[:,s],sem.at[0,t]),pltpu.make_async_copy(wu_h.at[L,:,s],wu.at[:,s],sem.at[1,t]),
                pltpu.make_async_copy(wd_h.at[L,s,:],wd.at[lax.rem(t,2)],sem.at[2,t])]
    @pl.when(j==0)
    def _():
        o.greet((o.partner,*o.upeer,*o.vpeer))
        for c in cps(0): c.start()
        for t in range(1,nf):
            for c in cps(t)[:2]: c.start()
        ss_ref[...]=jnp.zeros_like(ss_ref)
        for r in range(0,T,rc): aT[:,pl.ds(r,rc)]=a_ref[pl.ds(r,rc),:].T
    s=pl.ds(pl.multiple_of(lax.rem(j,nf)*ft,ft),ft)
    @pl.when(j<nf)
    def _():
        for c in cps(j): c.wait()
        @pl.when(j+1<nf)
        def _(): cps(j+1)[2].start()
        wgt,wut,wdt=wg[:,s],wu[:,s],wd[lax.rem(j,2)]
        for r in range(0,T,rc):
            rs_=pl.ds(r,rc); a=a_ref[rs_,:]
            g=dot(a,wgt); u=dot(a,wut); da=dot(dy_ref[rs_,:],wdt,NT).astype(BF).astype(F32)
            act[rs_,:],dg[rs_,s],du[rs_,s]=elementwise(g,u,da)
    @pl.when(j==0)
    def _(): pl.semaphore_wait(pltpu.get_barrier_semaphore(),1+len(o.upeer)+len(o.vpeer))
    point(2*j,0)
    @pl.when(j<nf)
    def _():
        sc.store(j,dot(aT[...],dg[:,s]),0)
        sc.store(j,dot(aT[...],du[:,s]),1)
        sc.store(j,dot(act[...],dy_ref[...],TN),2)
    @pl.when((j>=nf)&(j<nf+nb))
    def _():
        rs_=pl.ds(pl.multiple_of((j-nf)*bc,bc),bc)
        da=(dot(dg[rs_,:],wg[...],NT).astype(BF).astype(F32)+dot(du[rs_,:],wu[...],NT).astype(BF).astype(F32)).astype(BF).astype(F32)
        x=h_ref[...].astype(F32); scale=norm_scale(x)
        t=jnp.sum(da*x,-1,keepdims=True)*(1.0/D)
        dn=(da*scale-x*(scale*scale*scale*t)).astype(BF).astype(F32)
        dh_ref[...]=(dy_ref[rs_,:].astype(F32)+dn).astype(BF)
    point(2*j+1,1)
def k2(a1,dy,h1,wg,wu,wd,n,L,points,ft=256,rc=512,bc=256,nl=4,ns=3):
    T,D=a1.shape; F=wg.shape[2]; z=Shards(n,D,F,ft); nf=z.nf; nb=T//bc; S=z.side
    rs,ag=points; steps=max(nf+nb,max(t[-1] for t in rs+ag)//2+1); check_points(rs,nl,ns,0); check_gather(ag,[t[3] for t in rs]); nleft=max(nf-len(ag),1)
    back=pl.BlockSpec((bc,D),lambda j:(jnp.clip(j-nf,0,nb-1),0)); all_=lambda *s:pl.BlockSpec(s,lambda j:(0,)*len(s))
    return pl.pallas_call(functools.partial(k2_body,z=z,nl=nl,ns=ns,rc=rc,bc=bc,L=L,rs=rs,ag=ag),grid=(steps,),
        in_specs=[VM,VM,back,ANY,ANY,ANY],out_specs=[ANY,all_(*z.blk),all_(nleft,*z.blk),back],
        out_shape=[jax.ShapeDtypeStruct((2,nf,S,S,*z.blk),BF),jax.ShapeDtypeStruct(z.blk,F32),jax.ShapeDtypeStruct((nleft,*z.blk),BF),jax.ShapeDtypeStruct((T,D),BF)],
        scratch_shapes=[pltpu.VMEM((D,F),BF),pltpu.VMEM((D,F),BF),pltpu.VMEM((2,ft,D),BF),pltpu.VMEM((D,T),BF),
                        pltpu.VMEM((T,F),BF),pltpu.VMEM((T,F),BF),pltpu.VMEM((T,ft),BF),DMA((3,nf)),*Scatter.scratch(z,nl,ns),*Gather.scratch(z,max(len(ag),1))],
        compiler_params=pltpu.CompilerParams(vmem_limit_bytes=67043328,collective_id=1,has_side_effects=True),name="k2",
        cost_estimate=pl.CostEstimate(flops=16*T*D*F,bytes_accessed=30<<20,transcendentals=T*F))(a1,dy,h1,wg,wu,wd)

def k3_body(aT_h,dh_ref,g_ref,u_ref,wd_ref,ss_ref,left_ref,Q1_,P_out,f_ref,Q1,P_ref,aT,dg,du,act,sq,nsend,nplane,nc,nS,nR,gS,gR,oS,sem,*refs,z,nl,ns,rc,count,rs,ag,left,sqp):
    j=pl.program_id(0); D,T=aT.shape; nf,S=z.nf,z.side
    o=Place(S); sc=Scatter(z,o,nl,ns,refs[:Scatter.N])
    nleft=len(left); gl=Gather(z,o,nf-nleft,Q1,refs[Scatter.N:]) if nleft else None
    apart=[(a,b) for a in range(S) for b in range(S) if a or b]; plane=[o.dev(o.u+a,o.v+b) for a,b in apart]
    to=lambda k,here=False:[send(P_ref.at[k,o.v],P_ref.at[k,(o.v+S-d)%S if here else o.v],gS.at[k,d-1],gR.at[k,d-1],o.vpeer[d-1]) for d in range(1,S)]
    def done(k,g):
        w=g.astype(F32); sq[...]+=w*w
        P_ref[k,o.v]=g
    def hand(k):
        for d in to(k): d.start()
    def there(k):
        for d in to(k,True): d.wait()
        give(k).start()
    give=lambda k:pltpu.make_async_copy(P_ref.at[k],P_out.at[k],oS.at[k])
    def reduce_(p,parity):
        for i in (3,2,1,0): run([t[i] for t in rs],p,parity,lambda k:sc.step(i,k,done))
    def rest(p,parity):
        if nleft:
            for i in (4,3,2,1,0): run([t[i] for t in left],p,parity,lambda k:gl.step(i,k))
        run([t[1] for t in ag],p,parity,there)
        run([t[0] for t in ag],p,parity,hand)
    load=pltpu.make_async_copy(aT_h,aT,sem)
    def front(rows,b):
        for r in rows:
            rs_=pl.ds(r,rc)
            da=dot(dh_ref[rs_,:],wd_ref[...],NT).astype(BF).astype(F32)
            act[b,rs_,:],dg[b,rs_,:],du[b,rs_,:]=elementwise(g_ref[rs_,:],u_ref[rs_,:],da)
    def back(k,part,b):
        if part<2: sc.store(k,dot(aT[...],(dg,du)[part][b]),part)
        else: sc.store(k,dot(act[b],dh_ref[...],TN),2)
    rows=range(0,T,rc); half=len(rows)//2; b=lax.rem(j,2)
    @pl.when(j==0)
    def _():
        load.start()
        o.greet((o.partner,*plane))
        sq[...]=ss_ref[...]
        for k in range(nleft): gl.P[k,o.v]=left_ref[k]
        front(rows[:half],b)
    @pl.when((j>0)&(j<nf))
    def _():
        front(rows[:half],b); back(j-1,0,1-b)
    @pl.when(j==nf)
    def _(): back(j-1,0,1-b)
    @pl.when(j==0)
    def _(): pl.semaphore_wait(pltpu.get_barrier_semaphore(),1+len(plane))
    reduce_(2*j,0); rest(2*j,0)
    @pl.when(j==0)
    def _():
        front(rows[half:],b); load.wait()
    @pl.when((j>0)&(j<nf))
    def _():
        back(j-1,1,1-b); front(rows[half:],b); back(j-1,2,1-b)
    @pl.when(j==nf)
    def _(): back(j-1,1,1-b); back(j-1,2,1-b)
    p=2*j+1
    reduce_(p,1)
    def sums(buf,at,peers,b): return [send(nsend.at[b],buf.at[a],nS.at[b,i],nR.at[b,i],d) for i,(a,d) in enumerate(zip(at,peers))]
    hops=((nplane,o.u*S+o.v,plane,[(o.u+S-a)%S*S+(o.v+S-b)%S for a,b in apart],S*S),(nc,o.c,[o.partner],[1-o.c],2))
    for b_ in range(3):
        @pl.when(p==sqp[b_])
        def _(b=b_):
            if b==0: t=jnp.broadcast_to(jnp.sum(jnp.sum(sq[...],0,keepdims=True),1,keepdims=True),(8,128))
            else:
                buf,_,peers,at,k=hops[b-1]
                for d in sums(buf,at,peers,b-1): d.wait()
                t=buf[0]
                for i in range(1,k): t=t+buf[i]
            if b<2:
                buf,mine,peers,_,_=hops[b]
                nsend[b]=t; buf[mine]=t
                for d in sums(buf,[mine]*len(peers),peers,b): d.start()
            else: f_ref[...]=jnp.minimum(1.0,0.5*lax.rsqrt(t*(1.0/count)+1e-30))
    rest(p,1)
    @pl.when(j==pl.num_programs(0)-1)
    def _():
        for k in range(nf): give(k).wait()
def k3(a0T,dh,gate,up,wd,ss,left,Q1,n,L,count,points,ft=256,rc=512,nl=6,ns=4,nleft=2):
    D,T=a0T.shape; F=gate.shape[1]; z=Shards(n,D,F,ft); nf=z.nf; S=z.side
    rs,ag,lp,sqp=points; steps=max(max(t[-1] for t in rs+ag+lp),sqp[-1])//2+1
    assert len(lp)==nleft
    check_points(rs,nl,ns,1); check_gather(ag); check_gather(lp); assert all(a[0]>=r[3] for a,r in zip(ag,rs))
    cl=lambda j:jnp.minimum(j,nf-1); all_=lambda *s:pl.BlockSpec(s,lambda j:(0,)*len(s))
    col=lambda r:pl.BlockSpec((r,ft),lambda j:(0,cl(j)))
    return pl.pallas_call(functools.partial(k3_body,z=z,nl=nl,ns=ns,rc=rc,count=count,rs=rs,ag=ag,left=lp,sqp=sqp),grid=(steps,),
        in_specs=[ANY,VM,col(T),col(T),pl.BlockSpec((None,ft,D),lambda j:(L,cl(j),0)),VM,VM,ANY],
        out_specs=[ANY,all_(8,128),ANY],
        out_shape=[jax.ShapeDtypeStruct((nf,S,*z.blk),BF),jax.ShapeDtypeStruct((8,128),F32),jax.ShapeDtypeStruct(Q1.shape,BF)],input_output_aliases={7:2},
        scratch_shapes=[pltpu.VMEM((nf,S,*z.blk),BF),pltpu.VMEM((D,T),BF)]+[pltpu.VMEM((2,T,ft),BF)]*3+[pltpu.VMEM(z.blk,F32),pltpu.VMEM((2,8,128),F32),pltpu.VMEM((S*S,8,128),F32),
            pltpu.VMEM((2,8,128),F32),DMA((2,S*S)),DMA((2,S*S)),DMA((nf,S-1)),DMA((nf,S-1)),DMA((nf,)),DMA,*Scatter.scratch(z,nl,ns),*(Gather.scratch(z,nleft) if nleft else [])],
        compiler_params=pltpu.CompilerParams(vmem_limit_bytes=67043328,collective_id=2,has_side_effects=True),name="k3",
        cost_estimate=pl.CostEstimate(flops=8*T*D*F,bytes_accessed=10*T*F,transcendentals=T*F))(a0T,dh,gate,up,wd,ss,left,Q1)


def points(rows):
    return [[ord(c) - ord("0") for c in row] for row in rows.split(",")]


K2_POINTS = (points("1257,3479,569;,78;=,9:=?,;<?A,=>AG,?@EM,ACKO"), points("79=?A,9;?AE,;=AGK,=?EMQ,?AIMQ"))
K3_POINTS = (points("35:>,57<@,79>B,9;?G,;=AI,=?EO,?AKS,ACMU,CIQW"), points("QY,QY,QY,QY,QY,QY,SY,UY,W["), points("048<>,048=?,04:>@,06;@B"), points("WY[")[0])

def adam_body(f_ref,*refs,z,plan,ng,alias,sub,depth):
    gs,refs=refs[:ng],refs[ng:]; ins=refs[:9]; outs=refs[9+alias:18+alias]
    gb,refs=refs[18+alias],refs[19+alias:]; ib,ob,(isem,osem)=refs[:9],refs[9:18],refs[18:]
    S,ft,rg,rd,nf=z.side,z.ft,z.rg,z.rd,z.nf; rs=S//sub; hf=2*S; N=len(plan)*sub
    f=f_ref[0:1,0:1]; o=Place(S)
    places=[(l*2+h)*S+part if h is not None else o.place(l,*part) for l,h,part,_ in plan]
    def at(ref,q,t):
        p=sum(jnp.where(t//sub==k,place,0) for k,place in enumerate(places)); h=lax.rem(t,sub)
        if q%3<2: return ref.at[p,pl.ds(pl.multiple_of(h*(rs*rg),8),rs*rg)]
        return ref.at[p//hf,:,lax.rem(p,hf),pl.ds(pl.multiple_of(h*(rs*rd),8),rs*rd)]
    def reads(t):
        b=lax.rem(t,depth); return [pltpu.make_async_copy(at(ins[q],q,t),ib[q].at[b],isem.at[b,q]) for q in range(9)]
    def writes(t):
        b=lax.rem(t,depth); return [pltpu.make_async_copy(ob[q].at[b],at(outs[q],q,t),osem.at[b,q]) for q in range(9)]
    def gread(ref,part,t):
        b=lax.rem(t,depth); h=lax.rem(t,sub)
        src=(ref if part is None else ref.at[part[0],:,part[1]]).at[:,pl.ds(h*rs,rs)]
        return pltpu.make_async_copy(src,gb.at[b],isem.at[b,9])
    def fetch(t):
        for c in reads(t): c.start()
        for k,(_,h,part,a) in enumerate(plan):
            @pl.when(t//sub==k)
            def _(a=a,part=None if h is None else (h,part)): gread(gs[a],part,t).start()
    def one(g,w,m,v,wo,mo,vo,at):
        g=g.astype(F32)*f
        m=0.9*m[at]+0.1*g
        v=0.95*v[at]+0.05*g*g
        w=w[at].astype(F32)
        wo[at]=(w-0.02*(m*lax.rsqrt(v+1e-8)+0.1*w)).astype(BF); mo[at]=m; vo[at]=v
    for t in range(depth-1): fetch(jnp.int32(t))
    def unit(t,_):
        b=lax.rem(t,depth)
        @pl.when(t+depth-1<N)
        def _(): fetch(t+depth-1)
        for c in reads(t): c.wait()
        pltpu.make_async_copy(gb.at[b],gb.at[b],isem.at[b,9]).wait()
        @pl.when(t>=depth)
        def _():
            for c in writes(t-depth): c.wait()
        def tile(k,_):
            for r in range(rs):
                for q in range(3):
                    rows,cols=(rd,z.D) if q==2 else (rg,ft)
                    for c in range(0,cols,LANES):
                        g=gb[b,k,r,pl.ds(q*z.part+c//LANES*rows,rows),:]
                        at=(k,pl.ds(r*rows,rows),pl.ds(c,LANES)) if q==2 else (pl.ds(r*rows,rows),pl.ds(pl.multiple_of(k*ft+c,LANES),LANES))
                        one(g,*(ib[q+3*t_].at[b] for t_ in range(3)),*(ob[q+3*t_].at[b] for t_ in range(3)),at)
            return 0
        lax.fori_loop(0,nf,tile,0)
        for c in writes(t): c.start()
        return 0
    lax.fori_loop(0,N,unit,0)
    for t in range(max(N-depth,0),N):
        for c in writes(jnp.int32(t)): c.wait()
def adam(f,gs,plan,state,before,n,ft=256,sub=2,depth=3):
    S=round((n//2)**0.5); rows,F=state[0].shape[1:]; z=Shards(n,rows*2*S,F,ft); nf=z.nf; D=z.D
    rs=S//sub; alias=len(before); k=1+len(gs)+9; el=len(plan)*3*rows*F
    buf=lambda a,q:pltpu.VMEM((depth,rs*z.rg,F) if q%3<2 else (depth,nf,rs*z.rd,D),a.dtype)
    return pl.pallas_call(functools.partial(adam_body,z=z,plan=plan,ng=len(gs),alias=alias,sub=sub,depth=depth),
        in_specs=[VM]+[ANY]*(len(gs)+9+alias),out_specs=[ANY]*9,
        scratch_shapes=[pltpu.VMEM((depth,nf,rs,*z.blk),BF)]+[buf(a,q) for q,a in enumerate(state)]*2+[DMA((depth,10)),DMA((depth,9))],
        out_shape=[jax.ShapeDtypeStruct(a.shape,a.dtype) for a in state],input_output_aliases={k+q:q for q in range(alias)},
        compiler_params=pltpu.CompilerParams(vmem_limit_bytes=67043328),name="adamw",
        cost_estimate=pl.CostEstimate(flops=20*el,bytes_accessed=22*el,transcendentals=el))(f,*gs,*state,*before)

def solution(mesh):
    n=mesh.shape["dp"]; S=round((n//2)**0.5); hf=2*S
    at=lambda x,y,c:(x%S*S+y%S)*2+c
    def turn(d):
        return [(at(x,y,c),at(x+d*(1-c),y+d*c,c)) for x in range(S) for y in range(S) for c in range(2)]
    swap=[(i,i^1) for i in range(n)]
    def step(x,dy,*arrays):
        w,m,v=(arrays[i:i+3] for i in (0,3,6))
        L,D,F=w[0].shape; count=sum(a.size for a in w); nf=F//256; nleft=nf-len(K2_POINTS[1])
        gate,up,h1,a1,a0T=k1(x[0],*w)
        G1,ss,left,dh=k2(a1,dy[0],h1,*w,n,1,K2_POINTS)
        P,f,G1=k3(a0T,dh,gate,up,w[2],ss,left,G1,n,0,count,K3_POINTS,nleft=nleft)
        state=[a.reshape(L,nf,hf,-1,D) if k%3==2 else a.reshape(L*hf,-1,F) for k,a in enumerate((*w,*m,*v))]
        move=lambda a,p:lax.ppermute(a,"dp",p)
        near=[move(P,turn(d)) for d in range(1,S)]; theirs=move(P,swap)
        out=adam(f,[G1,P],[(1,h,q,0) for h in range(2) for q in range(S)]+[(0,None,(0,0),1)],state,[],n)
        near,theirs,out=lax.optimization_barrier((near,theirs,out))
        far=[move(a,swap) for a in near]
        out=adam(f,[theirs,*near],[(0,None,(1,0),0)]+[(0,None,(0,d),d) for d in range(1,S)],state,out,n)
        far,out=lax.optimization_barrier((far,out))
        out=adam(f,far,[(0,None,(1,d),d-1) for d in range(1,S)],state,out,n)
        return tuple(o.reshape(a.shape) for o,a in zip(out,arrays))
    P=PartitionSpec
    return jax.shard_map(step,mesh=mesh,in_specs=(P(("rep","dp"),None,None),)*2+(P(None,None,None),)*9,
        out_specs=(P("rep",None,None),)*9,check_vma=False)
```
